32 devices in a mesh: groups: 2 (over y), seq: 4 (over z), tensor: 4 (over x, core).
Axes of the slice: x: 2, y: 2, z: 4, core: 2. Of those that a mesh axis runs over, the one named last changes fastest.
Arguments:
- final_block_queries: bfloat16 [256, 8192], P(('groups', 'seq'), 'tensor'), parts along dimension 0, may hold values from -96 to 96
- final_block_keys: bfloat16 [256, 1024], P(('groups', 'seq'), 'tensor'), parts along dimension 0, may hold values from -16 to 16
- final_block_values: bfloat16 [256, 1024], P(('groups', 'seq'), 'tensor'), parts along dimension 0, may hold values from -6 to 6
- prompt_cached_keys: bfloat16 [12288, 1024], P(('groups', 'seq'), 'tensor'), parts along dimension 0, may hold values from -16 to 16
- prompt_cached_values: bfloat16 [12288, 1024], P(('groups', 'seq'), 'tensor'), parts along dimension 0, may hold values from -6 to 6
- paged_cache_pool: bfloat16 [256, 128, 2, 1024], P(('groups', 'seq'), None, None, 'tensor'), parts along dimension 0, may hold values from -16 to 16
- step_slot_queries: bfloat16 [32, 4, 8192], P(('groups', 'seq'), None, 'tensor'), parts along dimension 0, may hold values from -96 to 96
- step_token_keys: bfloat16 [32, 4, 1024], P(('groups', 'seq'), None, 'tensor'), parts along dimension 0, may hold values from -16 to 16
- step_token_values: bfloat16 [32, 4, 1024], P(('groups', 'seq'), None, 'tensor'), parts along dimension 0, may hold values from -6 to 6
- normed_step_inputs: bfloat16 [32, 4, 8192], P(('groups', 'seq'), None, 'tensor'), parts along dimension 0, may hold values from -6 to 6
- adapter_down_maps: bfloat16 [8192, 128], P('tensor'), may hold values from -0.0625 to 0.0625
- adapter_up_maps: bfloat16 [128, 8192], P(None, 'tensor'), may hold values from -1.5 to 1.5
- slot_request: int32 [32], P('groups'), parts along dimension 0, may hold values from 0 to 15, as said below
- request_page_table: int32 [32, 8], P('groups'), parts along dimension 0, may hold values from 0 to 127, as said below
- lengths: int32 [32], P('groups'), parts along dimension 0, may hold values from 2 to 1024, as said below
- request_adapter: int32 [32], P('groups'), parts along dimension 0, may hold values from 0 to 7
- request_rank: int32 [32], P('groups'), parts along dimension 0, may hold values from 4 to 16
Outputs:
- prefill_out: bfloat16 [256, 8192], P(('groups', 'seq'), 'tensor'), parts along dimension 0
- decode_out: bfloat16 [32, 4, 8192], P(('groups', 'seq'), None, 'tensor'), parts along dimension 0
The draws below stay inside these ranges and needn't reach their ends.
There are 2 independent parts, one for each index of `groups`. The reference program is written for one: setup_inputs(seed, part) draws one part's arguments, and reference() takes and returns one part's arrays. A program takes and returns all parts, laid end to end along the dimension named above; an argument that names none is the same for every part. Nothing has to cross between parts.
Inputs may be any that keep to these rules, and one draw needn't show every extreme that they name: A permutation: slot k serves request slot_request[k]; the owner of slots k * 4 to (k + 1) * 4 - 1 is owner k. `request_page_table`: every pool page is named exactly once. For every owner and every block of 32 pool pages (pages b * 32 to (b + 1) * 32 - 1), exactly 8 of the pages of that owner's requests lie in the block. `lengths`: some request has exactly 1024 cached tokens.
All inputs are finite; a program needn't handle non-finite values.
Results may differ from the reference program's by a relative error of at most 0.028.
Values may be sent and summed in bfloat16 or wider, within the bound.
No kernel may reach another device: no remote copies, remote signals or barrier semaphores. Data moves between devices by JAX's collectives and lax.ppermute only.
A program may use at most 128 MiB of HBM per device.

```python
import jax
import jax.numpy as jnp
from jax import lax

MODEL_WIDTH = 8192
QUERY_HEAD_COUNT = 64
KEY_HEAD_COUNT = 8
HEAD_SIZE = 128
ADAPTER_COUNT = 8
LARGEST_RANK = 16
DECODE_STEPS = 4
PAGE_TOKENS = 128
REQUEST_PAGES = 8
REQ_DEV = 4
BLOCK_TOKENS = 128
PROMPT_CACHED = 6144
SLOT_COUNT = 16
POOL_DEV = 32
POOL_PAGES = 128
CAP = 8


def shuffle_pool(subkey):
    return jax.random.permutation(subkey, POOL_DEV)


def page_tables(key):
    random_root_key = jax.random.fold_in(key, 7001)
    owner_total = SLOT_COUNT // REQ_DEV
    serving = jax.random.permutation(jax.random.fold_in(random_root_key, 1), SLOT_COUNT).astype(jnp.int32)
    slot_spot = jax.vmap(shuffle_pool)(jax.random.split(jax.random.fold_in(random_root_key, 2), owner_total))
    places = jax.vmap(shuffle_pool)(jax.random.split(jax.random.fold_in(random_root_key, 3), owner_total))
    holder = slot_spot // CAP
    within = slot_spot % CAP
    owner_ids = jnp.arange(owner_total, dtype=jnp.int32)[:, None]
    pool_place = places[holder, owner_ids * CAP + within]
    by_slot = (holder * POOL_DEV + pool_place).reshape(SLOT_COUNT, REQUEST_PAGES).astype(jnp.int32)
    page_rows = jnp.zeros((SLOT_COUNT, REQUEST_PAGES), jnp.int32).at[serving].set(by_slot)
    return (serving, page_rows)


def context_key_rows(key):
    random_root_key = jax.random.fold_in(key, 7501)
    output_rows = jnp.clip(3.0 * jax.random.normal(jax.random.fold_in(random_root_key, 1), (PROMPT_CACHED, KEY_HEAD_COUNT * HEAD_SIZE)), -16.0, 16.0)
    return output_rows


def pool_data(key):
    random_root_key = jax.random.fold_in(key, 7601)
    full_shape = (POOL_PAGES, PAGE_TOKENS, KEY_HEAD_COUNT * HEAD_SIZE)
    key_part = jnp.clip(3.0 * jax.random.normal(jax.random.fold_in(random_root_key, 1), full_shape), -16.0, 16.0)
    value_part = jnp.clip(jax.random.normal(jax.random.fold_in(random_root_key, 3), full_shape), -6.0, 6.0)
    return jnp.stack([key_part, value_part], axis=2)


def draw_prompt_cached_keys(key, part):
    return context_key_rows(key).astype(jnp.bfloat16)


def draw_final_block_queries(key, part):
    random_root_key = jax.random.fold_in(key, 7301)
    output_rows = jnp.clip(jax.random.normal(jax.random.fold_in(random_root_key, 1), (BLOCK_TOKENS, QUERY_HEAD_COUNT * HEAD_SIZE)), -6.0, 6.0)
    return output_rows.astype(jnp.bfloat16)


def draw_paged_cache_pool(key, part):
    return pool_data(key).astype(jnp.bfloat16)


def draw_step_slot_queries(key, part):
    random_root_key = jax.random.fold_in(key, 7701)
    full_shape = (SLOT_COUNT, DECODE_STEPS, QUERY_HEAD_COUNT * HEAD_SIZE)
    output_rows = jnp.clip(jax.random.normal(jax.random.fold_in(random_root_key, 1), full_shape), -6.0, 6.0)
    return output_rows.astype(jnp.bfloat16)


def draw_slot_request(key, part):
    serving, page_rows = page_tables(key)
    return serving


def draw_request_page_table(key, part):
    serving, page_rows = page_tables(key)
    return page_rows


def draw_lengths(key, part):
    random_root_key = jax.random.fold_in(key, 7101)
    longest = REQUEST_PAGES * PAGE_TOKENS
    drawn = jax.random.randint(jax.random.fold_in(random_root_key, 1), (SLOT_COUNT,), 2, longest + 1)
    chosen = jax.random.randint(jax.random.fold_in(random_root_key, 2), (), 0, SLOT_COUNT)
    return jnp.where(jnp.arange(SLOT_COUNT, dtype=jnp.int32) == chosen, longest, drawn).astype(jnp.int32)


def set_ends(values, stream_key, least, largest):
    dims = values.shape
    place = [jax.random.randint(jax.random.fold_in(stream_key, axis), (), 0, dims[axis]) for axis in range(len(dims))]
    values = values.at[tuple(place)].set(least)
    longest = dims.index(max(dims))
    place[longest] = (place[longest] + 1) % dims[longest]
    return values.at[tuple(place)].set(largest)


def block_levels(stream_key, dims, shards, low, high):
    level = 1.0
    for position, parts in shards:
        steps = jax.random.uniform(jax.random.fold_in(jax.random.fold_in(stream_key, 6), position), (parts,), jnp.float32, low / len(shards), high / len(shards))
        level = level * jnp.repeat(jnp.exp(steps), dims[position] // parts).reshape((-1,) + (1,) * (len(dims) - 1 - position))
    return level


def noise(own_key, dims, deviation, bound, cuts=(), held_as=jnp.bfloat16):
    loudness = block_levels(own_key, dims, cuts, -0.22, 0.18) if cuts else 1.0
    values = jax.random.normal(own_key, dims, jnp.float32) * deviation * loudness
    return jnp.minimum(jnp.maximum(values, -bound), bound).astype(held_as)


def setup_inputs(seed: int = 0, part: int = 0) -> dict:
    streams_of = jax.random.split(jax.random.key(seed), 18)
    part_splits = jax.random.split(jax.random.fold_in(streams_of[17], part), 18)
    return {
        "final_block_queries": draw_final_block_queries(jax.random.fold_in(jax.random.fold_in(streams_of[17], part), 71), part),
        "final_block_keys": noise(part_splits[1], (BLOCK_TOKENS, KEY_HEAD_COUNT * HEAD_SIZE), 3.0, 16.0, ((0, 4), (1, 4))),
        "final_block_values": noise(part_splits[2], (BLOCK_TOKENS, KEY_HEAD_COUNT * HEAD_SIZE), 1.0, 6.0, ((0, 4), (1, 4))),
        "prompt_cached_keys": draw_prompt_cached_keys(jax.random.fold_in(jax.random.fold_in(streams_of[17], part), 71), part),
        "prompt_cached_values": noise(part_splits[4], (PROMPT_CACHED, KEY_HEAD_COUNT * HEAD_SIZE), 1.0, 6.0, ((0, 4), (1, 4))),
        "paged_cache_pool": draw_paged_cache_pool(jax.random.fold_in(jax.random.fold_in(streams_of[17], part), 71), part),
        "step_slot_queries": draw_step_slot_queries(jax.random.fold_in(jax.random.fold_in(streams_of[17], part), 71), part),
        "step_token_keys": noise(part_splits[7], (SLOT_COUNT, DECODE_STEPS, KEY_HEAD_COUNT * HEAD_SIZE), 3.0, 16.0, ((0, 4), (2, 4))),
        "step_token_values": noise(part_splits[8], (SLOT_COUNT, DECODE_STEPS, KEY_HEAD_COUNT * HEAD_SIZE), 1.0, 6.0, ((0, 4), (2, 4))),
        "normed_step_inputs": noise(part_splits[9], (SLOT_COUNT, DECODE_STEPS, MODEL_WIDTH), 1.0, 6.0, ((0, 4), (2, 4))),
        "adapter_down_maps": noise(streams_of[10], (MODEL_WIDTH, ADAPTER_COUNT * LARGEST_RANK), MODEL_WIDTH ** -0.5, 0.0625, ((0, 4),)),
        "adapter_up_maps": noise(streams_of[11], (ADAPTER_COUNT * LARGEST_RANK, QUERY_HEAD_COUNT * HEAD_SIZE), LARGEST_RANK ** -0.5, 1.5, ((1, 4),)),
        "slot_request": draw_slot_request(jax.random.fold_in(jax.random.fold_in(streams_of[17], part), 71), part),
        "request_page_table": draw_request_page_table(jax.random.fold_in(jax.random.fold_in(streams_of[17], part), 71), part),
        "lengths": draw_lengths(jax.random.fold_in(jax.random.fold_in(streams_of[17], part), 71), part),
        "request_adapter": set_ends(jax.random.randint(part_splits[15], (SLOT_COUNT,), 0, ADAPTER_COUNT), jax.random.fold_in(part_splits[15], 1), 0, ADAPTER_COUNT - 1).astype(jnp.int32),
        "request_rank": set_ends(jax.random.randint(part_splits[16], (SLOT_COUNT,), LARGEST_RANK // 4, LARGEST_RANK + 1), jax.random.fold_in(part_splits[16], 1), LARGEST_RANK // 4, LARGEST_RANK).astype(jnp.int32),
    }


MASKED = -1.0e30


def softmax_rows(query_vectors, paged_key_rows, paged_value_rows, allowed):
    query_total_count = query_vectors.shape[0]
    heads_per_group = QUERY_HEAD_COUNT // KEY_HEAD_COUNT
    query_head_rows = query_vectors.reshape(query_total_count, KEY_HEAD_COUNT, heads_per_group, HEAD_SIZE).astype(jnp.float32)
    key_head_rows = paged_key_rows.reshape(-1, KEY_HEAD_COUNT, HEAD_SIZE).astype(jnp.float32)
    value_head_rows = paged_value_rows.reshape(-1, KEY_HEAD_COUNT, HEAD_SIZE).astype(jnp.float32)

    def single_head(kv_head):
        query_part = lax.dynamic_index_in_dim(query_head_rows, kv_head, 1, keepdims=False)
        key_part = lax.dynamic_index_in_dim(key_head_rows, kv_head, 1, keepdims=False)
        value_part = lax.dynamic_index_in_dim(value_head_rows, kv_head, 1, keepdims=False)
        scores = jnp.einsum("tgd,pd->gtp", query_part, key_part) * (HEAD_SIZE ** -0.5)
        scores = jnp.where(allowed[None], scores, MASKED)
        row_max = jnp.max(scores, axis=-1, keepdims=True)
        weights = jnp.where(allowed[None], jnp.exp(scores - row_max), 0.0)
        row_total = jnp.sum(weights, axis=-1)
        rounded = lax.optimization_barrier(weights.astype(jnp.bfloat16)).astype(jnp.float32)
        summed = jnp.einsum("gtp,pd->gtd", rounded, value_part)
        return summed / row_total[..., None]

    head_outputs = lax.map(single_head, jnp.arange(KEY_HEAD_COUNT, dtype=jnp.int32))
    return jnp.transpose(head_outputs, (2, 0, 1, 3)).reshape(query_total_count, QUERY_HEAD_COUNT * HEAD_SIZE).astype(jnp.bfloat16)


def reference(final_block_queries, final_block_keys, final_block_values, prompt_cached_keys, prompt_cached_values, paged_cache_pool, step_slot_queries, step_token_keys, step_token_values, normed_step_inputs, adapter_down_maps, adapter_up_maps, slot_request, request_page_table, lengths, request_adapter, request_rank):
    prefill_keys = jnp.concatenate([prompt_cached_keys, final_block_keys], axis=0)
    prefill_values = jnp.concatenate([prompt_cached_values, final_block_values], axis=0)
    spots = jnp.arange(PROMPT_CACHED + BLOCK_TOKENS, dtype=jnp.int32)
    key_pos = jnp.where(spots < PROMPT_CACHED, -1, spots - PROMPT_CACHED)
    block_rows = min(64, BLOCK_TOKENS)

    def run_block(row_start):
        query_rows = lax.dynamic_slice_in_dim(final_block_queries, row_start, block_rows, 0)
        row_pos = row_start + jnp.arange(block_rows, dtype=jnp.int32)
        allowed = key_pos[None, :] <= row_pos[:, None]
        return softmax_rows(query_rows, prefill_keys, prefill_values, allowed)

    starts = jnp.arange(BLOCK_TOKENS // block_rows, dtype=jnp.int32) * block_rows
    prefill_out = lax.map(run_block, starts).reshape(BLOCK_TOKENS, QUERY_HEAD_COUNT * HEAD_SIZE)

    reduced_rank_state = jnp.dot(normed_step_inputs.reshape(SLOT_COUNT * DECODE_STEPS, MODEL_WIDTH), adapter_down_maps, preferred_element_type=jnp.float32)
    adapters = request_adapter[slot_request]
    ranks = request_rank[slot_request]
    column_indices = jnp.arange(ADAPTER_COUNT * LARGEST_RANK, dtype=jnp.int32)
    rank_keep_mask = (column_indices[None, :] // LARGEST_RANK == adapters[:, None]) & (column_indices[None, :] % LARGEST_RANK < ranks[:, None])
    adapter_kept_rank = jnp.where(jnp.repeat(rank_keep_mask, DECODE_STEPS, axis=0), reduced_rank_state, 0.0).astype(jnp.bfloat16)
    raised_queries = jnp.dot(adapter_kept_rank, adapter_up_maps, preferred_element_type=jnp.float32)
    decode_q = (step_slot_queries.reshape(SLOT_COUNT * DECODE_STEPS, QUERY_HEAD_COUNT * HEAD_SIZE).astype(jnp.float32) + raised_queries).astype(jnp.bfloat16)
    decode_q = lax.optimization_barrier(decode_q).reshape(SLOT_COUNT, DECODE_STEPS, QUERY_HEAD_COUNT * HEAD_SIZE)

    cache_pos = jnp.arange(REQUEST_PAGES * PAGE_TOKENS, dtype=jnp.int32)
    step_pos = jnp.arange(DECODE_STEPS, dtype=jnp.int32)

    def one_slot(decode_slot_index):
        request = slot_request[decode_slot_index]
        slot_page_list = paged_cache_pool[request_page_table[request]]
        paged_key_rows = jnp.concatenate([slot_page_list[:, :, 0].reshape(REQUEST_PAGES * PAGE_TOKENS, KEY_HEAD_COUNT * HEAD_SIZE), step_token_keys[decode_slot_index]], axis=0)
        paged_value_rows = jnp.concatenate([slot_page_list[:, :, 1].reshape(REQUEST_PAGES * PAGE_TOKENS, KEY_HEAD_COUNT * HEAD_SIZE), step_token_values[decode_slot_index]], axis=0)
        cache_ok = jnp.broadcast_to(cache_pos[None, :] < lengths[request], (DECODE_STEPS, REQUEST_PAGES * PAGE_TOKENS))
        fresh_ok = step_pos[None, :] <= step_pos[:, None]
        allowed = jnp.concatenate([cache_ok, fresh_ok], axis=1)
        return softmax_rows(decode_q[decode_slot_index], paged_key_rows, paged_value_rows, allowed)

    decode_out = lax.map(one_slot, jnp.arange(SLOT_COUNT, dtype=jnp.int32))
    return prefill_out, decode_out
```

```python
import functools

import jax
import jax.numpy as jnp
from jax import lax
from jax.experimental import pallas as pl
from jax.experimental.pallas import tpu as pltpu
from jax.sharding import PartitionSpec as P

HEAD_SIZE = 128
LARGEST_RANK = 16
LANES = 128
MASKED = -1e30
FLOOR = -1e29
LOG2E = 1.4426950408889634
SCALE = HEAD_SIZE ** (-0.5) * LOG2E


VMEM = pl.BlockSpec(memory_space=pltpu.VMEM)
SMEM = pl.BlockSpec(memory_space=pltpu.SMEM)
ANY = pl.BlockSpec(memory_space=pl.ANY)


def dot_nt(a, b):
    return lax.dot_general(a, b, (((1,), (1,)), ((), ())), preferred_element_type=jnp.float32)


def dot(a, b):
    return jnp.dot(a, b, preferred_element_type=jnp.float32)


def split_three(x):
    high = x.astype(jnp.bfloat16)
    rest = x - high.astype(jnp.float32)
    mid = rest.astype(jnp.bfloat16)
    low = (rest - mid.astype(jnp.float32)).astype(jnp.bfloat16)
    return high, mid, low


def put_lse(columns, rows):
    lane = lax.broadcasted_iota(jnp.int32, (rows, LANES), 1)
    tile = jnp.zeros((rows, LANES), jnp.float32)
    for h, column in enumerate(columns):
        tile = jnp.where(lane == h, column, tile)
    return tile


def store_remote(out_ref, outs, columns, rows):
    heads = len(outs)
    for h, value in enumerate(outs):
        out_ref[:, h * HEAD_SIZE : (h + 1) * HEAD_SIZE] = value.astype(jnp.bfloat16)
    lane = lax.broadcasted_iota(jnp.int32, (rows, LANES), 1)
    tile = jnp.zeros((rows, LANES), jnp.float32)
    for h, column in enumerate(columns):
        for piece, part in enumerate(split_three(column)):
            tile = jnp.where(lane == piece * heads + h, part.astype(jnp.float32), tile)
    out_ref[:, heads * HEAD_SIZE :] = tile.astype(jnp.bfloat16)


def store_own(out_ref, lse_ref, outs, columns, rows):
    for h, value in enumerate(outs):
        out_ref[:, h * HEAD_SIZE : (h + 1) * HEAD_SIZE] = value
    lse_ref[...] = put_lse(columns, rows)


def finish(total, summed, row_max):
    safe = jnp.where(total > 0.0, total, 1.0)
    lse = jnp.where(total > 0.0, row_max + jnp.log2(safe), MASKED)
    return summed * (1.0 / safe), lse


def prefill_kernel(kinds, allow_ref, *refs):
    count = len(kinds)
    q_refs = refs[:count]
    k_ref, v_ref, fresh_k_ref, fresh_v_ref = refs[count : count + 4]
    out_refs = list(refs[count + 4 :])
    kv_heads = k_ref.shape[1] // HEAD_SIZE
    for index, kind in enumerate(kinds):
        q_ref = q_refs[index]
        rows = q_ref.shape[0]
        fresh = fresh_k_ref.shape[0]
        heads = q_ref.shape[1] // HEAD_SIZE
        group = heads // kv_heads
        outs, columns = [], []
        for g in range(kv_heads):
            lanes = slice(g * HEAD_SIZE, (g + 1) * HEAD_SIZE)
            query = jnp.concatenate(
                [
                    q_ref[:, (g * group + i) * HEAD_SIZE : (g * group + i + 1) * HEAD_SIZE]
                    for i in range(group)
                ],
                axis=0,
            )
            scores = dot_nt(query, k_ref[:, lanes]) * SCALE
            fresh_scores = dot_nt(query, fresh_k_ref[:, lanes]) * SCALE
            shape = (group * rows, fresh)
            if kind == "own":
                row = lax.broadcasted_iota(jnp.int32, shape, 0) % rows
                ok = lax.broadcasted_iota(jnp.int32, shape, 1) <= row
            else:
                ok = lax.broadcasted_iota(jnp.int32, shape, 0) < allow_ref[index] * group * rows
            fresh_scores = jnp.where(ok, fresh_scores, MASKED)
            row_max = jnp.maximum(
                jnp.max(scores, axis=1, keepdims=True), jnp.max(fresh_scores, axis=1, keepdims=True)
            )
            weights = jnp.exp2(scores - row_max)
            fresh_weights = jnp.where(ok, jnp.exp2(fresh_scores - row_max), 0.0)
            total = jnp.sum(weights, axis=1, keepdims=True) + jnp.sum(
                fresh_weights, axis=1, keepdims=True
            )
            summed = dot(weights.astype(jnp.bfloat16), v_ref[:, lanes]) + dot(
                fresh_weights.astype(jnp.bfloat16), fresh_v_ref[:, lanes]
            )
            result, lse = finish(total, summed, row_max)
            for i in range(group):
                outs.append(result[i * rows : (i + 1) * rows])
                columns.append(lse[i * rows : (i + 1) * rows])
        if kind == "own":
            store_own(out_refs.pop(0), out_refs.pop(0), outs, columns, rows)
        else:
            store_remote(out_refs.pop(0), outs, columns, rows)


def out_shapes(kinds, rows, width):
    shapes = []
    for kind in kinds:
        if kind == "own":
            shapes.append(jax.ShapeDtypeStruct((rows, width), jnp.float32))
            shapes.append(jax.ShapeDtypeStruct((rows, LANES), jnp.float32))
        else:
            shapes.append(jax.ShapeDtypeStruct((rows, width + LANES), jnp.bfloat16))
    return shapes


def prefill_part(kinds, allow, queries, keys, values, fresh_keys, fresh_values):
    rows, width = queries[0].shape
    shapes = out_shapes(kinds, rows, width)
    heads = width // HEAD_SIZE
    work = len(kinds) * rows * heads * (keys.shape[0] + fresh_keys.shape[0])
    return pl.pallas_call(
        functools.partial(prefill_kernel, kinds),
        out_shape=shapes,
        in_specs=[SMEM] + [VMEM] * (len(queries) + 4),
        out_specs=[VMEM] * len(shapes),
        cost_estimate=pl.CostEstimate(
            flops=work * HEAD_SIZE * 4, bytes_accessed=keys.size * 4, transcendentals=work
        ),
        name="prefill_" + "_".join(kinds),
    )(allow, *queries, keys, values, fresh_keys, fresh_values)


def decode_kernel(kinds, offsets, me_ref, request_ref, table_ref, lengths_ref, *refs):
    count = len(kinds)
    q_refs = refs[:count]
    pool_ref, fresh_k_ref, fresh_v_ref = refs[count : count + 3]
    pages_ref, slot_ref, valid_ref, buf_ref, sem = refs[-5:]
    out_refs = list(refs[count + 3 : -5])
    pool_here, page_len = pool_ref.shape[0], pool_ref.shape[1]
    kv_heads = pool_ref.shape[3] // HEAD_SIZE
    slots_here, steps = fresh_k_ref.shape[0], fresh_k_ref.shape[1]
    page_count = table_ref.shape[1]
    per_owner = buf_ref.shape[0] // count
    rows = slots_here * steps
    me = me_ref[0]

    for index in range(count):
        owner = lax.bitwise_xor(me, offsets[index])

        def find(entry, found):
            slot = entry // page_count
            place = entry - slot * page_count
            request = request_ref[owner * slots_here + slot]
            page = table_ref[request, place]
            local = page - me * pool_here
            mine = (local >= 0) & (local < pool_here)
            left = lengths_ref[request] - place * page_len

            @pl.when(mine)
            def _():
                spot = index * per_owner + found
                pages_ref[spot] = local
                slot_ref[spot] = slot
                valid_ref[spot] = jnp.clip(left, 0, page_len)
                pltpu.make_async_copy(pool_ref.at[local], buf_ref.at[spot], sem.at[index]).start()

            return found + mine.astype(jnp.int32)

        lax.fori_loop(0, slots_here * page_count, find, jnp.int32(0))

    for index, kind in enumerate(kinds):
        q_ref = q_refs[index]
        heads = q_ref.shape[1] // HEAD_SIZE
        group = heads // kv_heads
        total_rows = group * rows
        block = buf_ref.at[pl.ds(index * per_owner, per_owner)]
        pltpu.make_async_copy(block, block, sem.at[index]).wait()
        row_slot = (lax.broadcasted_iota(jnp.int32, (total_rows, 1), 0) % rows) // steps
        column = lax.broadcasted_iota(jnp.int32, (1, 2 * page_len), 1)
        spot_of = jnp.where(column % 2 == 0, column // 2, page_len)
        outs, columns = [], []
        for g in range(kv_heads):
            lanes = slice(g * HEAD_SIZE, (g + 1) * HEAD_SIZE)
            query = jnp.concatenate(
                [
                    q_ref[:, (g * group + i) * HEAD_SIZE : (g * group + i + 1) * HEAD_SIZE]
                    for i in range(group)
                ],
                axis=0,
            )
            parts = []
            row_max = jnp.full((total_rows, 1), FLOOR, jnp.float32)
            for j in range(per_owner):
                spot = index * per_owner + j
                both = buf_ref.at[spot].reshape(2 * page_len, buf_ref.shape[3])[:, lanes]
                scores = dot_nt(query, both) * SCALE
                limit = jnp.where(row_slot == slot_ref[spot], valid_ref[spot], 0)
                scores = jnp.where(spot_of < limit, scores, MASKED)
                row_max = jnp.maximum(row_max, jnp.max(scores, axis=1, keepdims=True))
                parts.append((scores, both))
            if kind == "own":
                fresh_keys = fresh_k_ref[...].reshape(rows, -1)[:, lanes]
                fresh_values = fresh_v_ref[...].reshape(rows, -1)[:, lanes]
                scores = dot_nt(query, fresh_keys) * SCALE
                shape = (total_rows, rows)
                row = lax.broadcasted_iota(jnp.int32, shape, 0) % rows
                col = lax.broadcasted_iota(jnp.int32, shape, 1)
                ok = (row // steps == col // steps) & (col % steps <= row % steps)
                scores = jnp.where(ok, scores, MASKED)
                row_max = jnp.maximum(row_max, jnp.max(scores, axis=1, keepdims=True))
                weights = jnp.exp2(scores - row_max)
                total = jnp.sum(weights, axis=1, keepdims=True)
                summed = dot(weights.astype(jnp.bfloat16), fresh_values)
            else:
                total = jnp.zeros((total_rows, 1), jnp.float32)
                summed = jnp.zeros((total_rows, HEAD_SIZE), jnp.float32)
            for scores, both in parts:
                weights = jnp.exp2(scores - row_max)
                total = total + jnp.sum(weights, axis=1, keepdims=True)
                shifted = pltpu.roll(weights, 1, 1)
                summed = summed + dot(shifted.astype(jnp.bfloat16), both)
            result, lse = finish(total, summed, row_max)
            for i in range(group):
                outs.append(result[i * rows : (i + 1) * rows])
                columns.append(lse[i * rows : (i + 1) * rows])
        if kind == "own":
            store_own(out_refs.pop(0), out_refs.pop(0), outs, columns, rows)
        else:
            store_remote(out_refs.pop(0), outs, columns, rows)


def decode_part(kinds, offsets, seq_count, me, request, table, lengths, queries, pool, fresh_keys, fresh_values):
    rows, width = queries[0].shape
    shapes = out_shapes(kinds, rows, width)
    heads = width // HEAD_SIZE
    slots_here = fresh_keys.shape[0]
    per_owner = slots_here * table.shape[1] // seq_count
    spots = len(kinds) * per_owner
    work = len(kinds) * rows * heads * per_owner * pool.shape[1] * 2
    return pl.pallas_call(
        functools.partial(decode_kernel, kinds, offsets),
        out_shape=shapes,
        in_specs=[SMEM] * 4 + [VMEM] * len(queries) + [ANY, VMEM, VMEM],
        out_specs=[VMEM] * len(shapes),
        scratch_shapes=[
            pltpu.SMEM((spots,), jnp.int32),
            pltpu.SMEM((spots,), jnp.int32),
            pltpu.SMEM((spots,), jnp.int32),
            pltpu.VMEM((spots,) + pool.shape[1:], jnp.bfloat16),
            pltpu.SemaphoreType.DMA((len(kinds),)),
        ],
        cost_estimate=pl.CostEstimate(
            flops=work * HEAD_SIZE * 4, bytes_accessed=pool.size * 2, transcendentals=work
        ),
        name="decode_" + "_".join(kinds),
    )(me, request, table, lengths, *queries, pool, fresh_keys, fresh_values)


def combine_kernel(own_ref, own_lse_ref, *refs):
    chunk_refs, out_ref = refs[:-1], refs[-1]
    heads = own_ref.shape[1] // HEAD_SIZE
    width = heads * HEAD_SIZE
    lses = [own_lse_ref[:, :heads]]
    for ref in chunk_refs:
        tile = ref[:, width:].astype(jnp.float32)
        lses.append(
            tile[:, :heads] + tile[:, heads : 2 * heads] + tile[:, 2 * heads : 3 * heads]
        )
    best = functools.reduce(jnp.maximum, lses)
    factors = [jnp.exp2(lse - best) for lse in lses]
    inverse = 1.0 / functools.reduce(jnp.add, factors)
    factors = [factor * inverse for factor in factors]
    for h in range(heads):
        lanes = slice(h * HEAD_SIZE, (h + 1) * HEAD_SIZE)
        merged = own_ref[:, lanes] * factors[0][:, h : h + 1]
        for ref, factor in zip(chunk_refs, factors[1:]):
            merged = merged + ref[:, lanes].astype(jnp.float32) * factor[:, h : h + 1]
        out_ref[:, lanes] = merged.astype(jnp.bfloat16)


def combine(own, own_lse, chunks):
    return pl.pallas_call(
        combine_kernel,
        out_shape=jax.ShapeDtypeStruct(own.shape, jnp.bfloat16),
        in_specs=[VMEM] * (2 + len(chunks)),
        out_specs=VMEM,
        cost_estimate=pl.CostEstimate(
            flops=own.size * 2 * (1 + len(chunks)), bytes_accessed=own.size * 8, transcendentals=0
        ),
        name="combine",
    )(own, own_lse, *chunks)


def adapter_kernel(me_ref, request_ref, adapter_ref, rank_ref, low_ref, up_ref, base_ref, out_ref):
    slots_here, steps = base_ref.shape[0], base_ref.shape[1]
    rows = slots_here * steps
    shape = low_ref.shape
    row_slot = lax.broadcasted_iota(jnp.int32, shape, 0) // steps
    column = lax.broadcasted_iota(jnp.int32, shape, 1)
    first = jnp.zeros(shape, jnp.int32)
    last = jnp.zeros(shape, jnp.int32)
    for slot in range(slots_here):
        request = request_ref[me_ref[0] * slots_here + slot]
        start = adapter_ref[request] * LARGEST_RANK
        first = jnp.where(row_slot == slot, start, first)
        last = jnp.where(row_slot == slot, start + jnp.minimum(rank_ref[request], LARGEST_RANK), last)
    kept = jnp.where((column >= first) & (column < last), low_ref[...], 0.0).astype(jnp.bfloat16)
    raised = dot(kept, up_ref[...])
    base = base_ref[...].astype(jnp.float32).reshape(rows, base_ref.shape[2])
    out_ref[...] = (base + raised).astype(jnp.bfloat16)


def adapter_queries(me, request, adapter, rank, low, up, base):
    rows = base.shape[0] * base.shape[1]
    return pl.pallas_call(
        adapter_kernel,
        out_shape=jax.ShapeDtypeStruct((rows, base.shape[2]), jnp.bfloat16),
        in_specs=[SMEM] * 4 + [VMEM] * 3,
        out_specs=VMEM,
        cost_estimate=pl.CostEstimate(
            flops=2 * rows * up.size, bytes_accessed=up.size * 2, transcendentals=0
        ),
        name="adapter",
    )(me, request, adapter, rank, low, up, base)


def exchange(x, axis, offset):
    count = lax.axis_size(axis)
    return lax.ppermute(x, axis, [(i, i ^ offset) for i in range(count)])


def per_device(
    final_block_queries,
    final_block_keys,
    final_block_values,
    prompt_cached_keys,
    prompt_cached_values,
    paged_cache_pool,
    step_slot_queries,
    step_token_keys,
    step_token_values,
    normed_step_inputs,
    adapter_down_maps,
    adapter_up_maps,
    slot_request,
    request_page_table,
    lengths,
    request_adapter,
    request_rank,
):
    seq_count = lax.axis_size("seq")
    tensor_count = lax.axis_size("tensor")
    position = lax.axis_index("seq").astype(jnp.int32)
    me = position.reshape(1)
    offsets = list(range(2, seq_count)) + [1]
    arrived = {o: exchange(final_block_queries, "seq", o) for o in offsets}

    slots_here, steps, width = step_slot_queries.shape
    low = jnp.dot(
        normed_step_inputs.reshape(slots_here * steps, -1),
        adapter_down_maps,
        preferred_element_type=jnp.float32,
    )
    bit = 1
    while bit < tensor_count:
        low = low + exchange(low, "tensor", bit)
        bit *= 2
    decode_queries = adapter_queries(
        me, slot_request, request_adapter, request_rank, low, adapter_up_maps, step_slot_queries
    )
    decode_arrived = {o: exchange(decode_queries, "seq", o) for o in offsets}

    shared = (prompt_cached_keys, prompt_cached_values, final_block_keys, final_block_values)
    none = jnp.zeros((1,), jnp.int32)
    own, own_lse = prefill_part(("own",), none, [final_block_queries], *shared)
    returned = []
    for o in offsets:
        allow = ((position ^ o) > position).astype(jnp.int32).reshape(1)
        (part,) = prefill_part(("far",), allow, [arrived[o]], *shared)
        returned.append(exchange(part, "seq", o))

    kinds = ("own",) + ("far",) * len(offsets)
    parts = decode_part(
        kinds,
        (0,) + tuple(offsets),
        seq_count,
        me,
        slot_request,
        request_page_table,
        lengths,
        [decode_queries] + [decode_arrived[o] for o in offsets],
        paged_cache_pool,
        step_token_keys,
        step_token_values,
    )
    decode_returned = [exchange(part, "seq", o) for part, o in zip(parts[2:], offsets)]

    prefill_out = combine(own, own_lse, returned)
    decode_out = combine(parts[0], parts[1], decode_returned)
    return (prefill_out, decode_out.reshape(slots_here, steps, width))


def solution(mesh):
    placed = (
        P(("groups", "seq"), "tensor"),
        P(("groups", "seq"), "tensor"),
        P(("groups", "seq"), "tensor"),
        P(("groups", "seq"), "tensor"),
        P(("groups", "seq"), "tensor"),
        P(("groups", "seq"), None, None, "tensor"),
        P(("groups", "seq"), None, "tensor"),
        P(("groups", "seq"), None, "tensor"),
        P(("groups", "seq"), None, "tensor"),
        P(("groups", "seq"), None, "tensor"),
        P("tensor", None),
        P(None, "tensor"),
        P("groups"),
        P("groups", None),
        P("groups"),
        P("groups"),
        P("groups"),
    )
    return jax.shard_map(
        per_device,
        mesh=mesh,
        in_specs=placed,
        out_specs=(P(("groups", "seq"), "tensor"), P(("groups", "seq"), None, "tensor")),
        check_vma=False,
    )
```

```python
import functools

import jax
import jax.numpy as jnp
from jax import lax
from jax.experimental import pallas as pl
from jax.experimental.pallas import tpu as pltpu
from jax.sharding import PartitionSpec as P

HEAD_SIZE = 128
LARGEST_RANK = 16
LANES = 128
MIB = 1 << 20
MASKED = -1e30
FLOOR = -1e29
SCALE = HEAD_SIZE ** (-0.5)


VMEM = pl.BlockSpec(memory_space=pltpu.VMEM)
SMEM = pl.BlockSpec(memory_space=pltpu.SMEM)
HBM = pl.BlockSpec(memory_space=pltpu.HBM)


def dot_nt(a, b):
    return lax.dot_general(a, b, (((1,), (1,)), ((), ())), preferred_element_type=jnp.float32)


def dot(a, b):
    return jnp.dot(a, b, preferred_element_type=jnp.float32)


def split_three(x):
    high = x.astype(jnp.bfloat16)
    rest = x - high.astype(jnp.float32)
    mid = rest.astype(jnp.bfloat16)
    low = (rest - mid.astype(jnp.float32)).astype(jnp.bfloat16)
    return high, mid, low


def put_lse(columns, rows):
    lane = lax.broadcasted_iota(jnp.int32, (rows, LANES), 1)
    tile = jnp.zeros((rows, LANES), jnp.float32)
    for h, column in enumerate(columns):
        tile = jnp.where(lane == h, column, tile)
    return tile


def split_lse(columns, rows):
    lane = lax.broadcasted_iota(jnp.int32, (rows, LANES), 1)
    count = len(columns)
    whole = put_lse(columns, rows)
    pieces = [piece.astype(jnp.float32) for piece in split_three(whole)]
    tile = pieces[0]
    for index in (1, 2):
        moved = pltpu.roll(pieces[index], index * count, 1)
        tile = jnp.where(lane >= index * count, moved, tile)
    return tile.astype(jnp.bfloat16)


def join_lse(tile, count):
    tile = tile.astype(jnp.float32)
    return tile[:, :count] + tile[:, count : 2 * count] + tile[:, 2 * count : 3 * count]


def merge_factors(lses):
    best = functools.reduce(jnp.maximum, lses)
    factors = [jnp.exp(lse - best) for lse in lses]
    inverse = 1.0 / functools.reduce(jnp.add, factors)
    return [factor * inverse for factor in factors]


def store_remote(out_ref, outs, columns, rows):
    heads = len(outs)
    for h, value in enumerate(outs):
        out_ref[:, h * HEAD_SIZE : (h + 1) * HEAD_SIZE] = value.astype(jnp.bfloat16)
    out_ref[:, heads * HEAD_SIZE :] = split_lse(columns, rows)


def store_own(out_ref, lse_ref, outs, columns, rows):
    for h, value in enumerate(outs):
        out_ref[:, h * HEAD_SIZE : (h + 1) * HEAD_SIZE] = value
    lse_ref[...] = put_lse(columns, rows)


def finish(total, summed, row_max):
    safe = jnp.where(total > 0.0, total, 1.0)
    lse = jnp.where(total > 0.0, row_max * SCALE + jnp.log(safe), MASKED)
    return summed * (1.0 / safe), lse


def fetch_pages(
    owners, me_ref, request_ref, table_ref, pool_ref, pages_ref, entry_ref, place_ref, sem, slots_here
):
    pool_here, page_len = pool_ref.shape[0], pool_ref.shape[1]
    kv_heads = pool_ref.shape[3] // HEAD_SIZE
    page_count = table_ref.shape[0]
    first, count = owners
    per_owner = pages_ref.shape[1] // count
    me = me_ref[0]

    def fetch(index, carry):
        owner = lax.bitwise_xor(me, first + index)
        found = index * (per_owner + 1)
        last = found + per_owner
        for slot in range(slots_here):
            request = request_ref[owner * slots_here + slot]
            for place in range(page_count):
                local = table_ref[place, request] - me * pool_here
                place_ref[found] = local
                entry_ref[found] = slot * page_count + place
                mine = (local >= 0) & (local < pool_here)
                found = jnp.minimum(found + mine.astype(jnp.int32), last)
        for j in range(per_owner):
            local = place_ref[index * (per_owner + 1) + j]
            page = pool_ref.at[local].reshape(2 * page_len, pool_ref.shape[3])
            for g in range(kv_heads):
                pltpu.make_async_copy(
                    page.at[:, pl.ds(g * HEAD_SIZE, HEAD_SIZE)],
                    pages_ref.at[g, index * per_owner + j],
                    sem,
                ).start()
        return carry

    if count <= 4:
        for index in range(count):
            fetch(index, 0)
    else:
        lax.fori_loop(0, count, fetch, 0)


def prefill_rows(kind, allow, q_ref, k_ref, v_ref, fresh_k_ref, fresh_v_ref):
    rows = q_ref.shape[0]
    fresh = fresh_k_ref.shape[0]
    kv_heads = k_ref.shape[1] // HEAD_SIZE
    group = q_ref.shape[1] // HEAD_SIZE // kv_heads
    outs, columns = [], []
    for g in range(kv_heads):
        lanes = slice(g * HEAD_SIZE, (g + 1) * HEAD_SIZE)
        query = jnp.concatenate(
            [
                q_ref[:, (g * group + i) * HEAD_SIZE : (g * group + i + 1) * HEAD_SIZE]
                for i in range(group)
            ],
            axis=0,
        )
        scores = dot_nt(query, k_ref[:, lanes])
        fresh_scores = dot_nt(query, fresh_k_ref[:, lanes])
        shape = (group * rows, fresh)
        row = lax.broadcasted_iota(jnp.int32, shape, 0)
        if kind == "own":
            ok = lax.broadcasted_iota(jnp.int32, shape, 1) <= row % rows
        else:
            ok = row < allow * group * rows
        fresh_scores = jnp.where(ok, fresh_scores, MASKED)
        row_max = jnp.maximum(
            jnp.max(scores, axis=1, keepdims=True), jnp.max(fresh_scores, axis=1, keepdims=True)
        )
        weights = jnp.exp((scores - row_max) * SCALE)
        fresh_weights = jnp.where(ok, jnp.exp((fresh_scores - row_max) * SCALE), 0.0)
        total = jnp.sum(weights, axis=1, keepdims=True) + jnp.sum(
            fresh_weights, axis=1, keepdims=True
        )
        summed = dot(weights.astype(jnp.bfloat16), v_ref[:, lanes]) + dot(
            fresh_weights.astype(jnp.bfloat16), fresh_v_ref[:, lanes]
        )
        result, lse = finish(total, summed, row_max)
        for i in range(group):
            outs.append(result[i * rows : (i + 1) * rows])
            columns.append(lse[i * rows : (i + 1) * rows])
    return outs, columns


def prefill_kernel(kind, allow_ref, q_ref, k_ref, v_ref, fresh_k_ref, fresh_v_ref, *refs):
    rows = q_ref.shape[0]
    outs, columns = prefill_rows(
        kind, allow_ref[0], q_ref, k_ref, v_ref, fresh_k_ref, fresh_v_ref
    )
    if kind == "own":
        store_own(refs[0], refs[1], outs, columns, rows)
    else:
        store_remote(refs[0], outs, columns, rows)


def prefill_fetch_kernel(owners, slots_here, load_count, allow_ref, q_ref, *refs):
    if load_count:
        sources, refs = refs[:load_count], refs[load_count:]
    else:
        loaded, refs = refs[:4], refs[4:]
    (me_ref, request_ref, table_ref, pool_ref), refs = refs[:4], refs[4:]
    if load_count:
        loaded, refs = refs[:load_count], refs[load_count:]
    out_ref, pages_ref, entry_ref, place_ref, sem, load_sem = refs
    copies = []
    if load_count:
        copies = [
            pltpu.make_async_copy(source, target, load_sem.at[i])
            for i, (source, target) in enumerate(zip(sources, loaded))
        ]
        for copy in copies:
            copy.start()
    fetch_pages(
        owners, me_ref, request_ref, table_ref, pool_ref, pages_ref, entry_ref, place_ref, sem,
        slots_here,
    )
    for copy in copies:
        copy.wait()
    prefill_kernel("far", allow_ref, q_ref, *loaded[:4], out_ref)
    pltpu.make_async_copy(pages_ref, pages_ref, sem).wait()


def prefill_cost(queries, keys, fresh_keys):
    work = queries.size // HEAD_SIZE * (keys.shape[0] + fresh_keys.shape[0])
    return pl.CostEstimate(
        flops=work * HEAD_SIZE * 4, bytes_accessed=keys.size * 4, transcendentals=work
    )


def prefill_part(kind, allow, queries, keys, values, fresh_keys, fresh_values):
    rows, width = queries.shape
    if kind == "own":
        shapes = [
            jax.ShapeDtypeStruct((rows, width), jnp.float32),
            jax.ShapeDtypeStruct((rows, LANES), jnp.float32),
        ]
    else:
        shapes = [jax.ShapeDtypeStruct((rows, width + LANES), jnp.bfloat16)]
    return pl.pallas_call(
        functools.partial(prefill_kernel, kind),
        out_shape=shapes,
        in_specs=[SMEM] + [VMEM] * 5,
        out_specs=[VMEM] * len(shapes),
        compiler_params=pltpu.CompilerParams(vmem_limit_bytes=16 * MIB),
        cost_estimate=prefill_cost(queries, keys, fresh_keys),
        name="prefill_" + kind,
    )(allow, queries, keys, values, fresh_keys, fresh_values)


def prefill_fetch(owners, slots_here, allow, queries, shared, load, me, request, table, pool):
    rows, width = queries.shape
    spots = slots_here * table.shape[0] * slots_here // request.shape[0] * owners[1]
    keys, fresh_keys = (load or shared)[0], (load or shared)[2]
    arrays = load or shared
    return pl.pallas_call(
        functools.partial(prefill_fetch_kernel, owners, slots_here, len(load)),
        out_shape=[jax.ShapeDtypeStruct(x.shape, x.dtype) for x in load]
        + [
            jax.ShapeDtypeStruct((rows, width + LANES), jnp.bfloat16),
            jax.ShapeDtypeStruct(
                (pool.shape[3] // HEAD_SIZE, spots, 2 * pool.shape[1], HEAD_SIZE), jnp.bfloat16
            ),
            jax.ShapeDtypeStruct((spots + owners[1],), jnp.int32),
        ],
        in_specs=[SMEM, VMEM] + [HBM if load else VMEM] * len(arrays) + [SMEM] * 3 + [HBM],
        out_specs=[VMEM] * (len(load) + 2) + [SMEM],
        scratch_shapes=[
            pltpu.SMEM((spots + owners[1],), jnp.int32),
            pltpu.SemaphoreType.DMA,
            pltpu.SemaphoreType.DMA((max(1, len(load)),)),
        ],
        compiler_params=pltpu.CompilerParams(vmem_limit_bytes=16 * MIB),
        cost_estimate=prefill_cost(queries, keys, fresh_keys),
        name="prefill_fetch",
    )(allow, queries, *arrays, me, request, table, pool)


def decode_kernel(halves, me_ref, request_ref, lengths_ref, *refs):
    entry_refs, refs = refs[: len(halves)], refs[len(halves) :]
    count = sum(halves)
    q_refs, refs = refs[:count], refs[count:]
    pages_refs, refs = refs[: len(halves)], refs[len(halves) :]
    fresh_k_ref, fresh_v_ref, own_ref, own_lse_ref = refs[:4]
    out_refs = refs[4:]
    kv_heads, spots, twice = pages_refs[0].shape[:3]
    page_len = twice // 2
    slots_here, steps = fresh_k_ref.shape[0], fresh_k_ref.shape[1]
    per_owner = spots // halves[0]
    page_count = per_owner * count // slots_here
    rows = q_refs[0].shape[0] // (kv_heads * slots_here)
    fresh = slots_here * steps
    column = lax.broadcasted_iota(jnp.int32, (1, twice), 1)
    spot_of = jnp.where(column % 2 == 0, column // 2, page_len)
    fresh_keys = fresh_k_ref[...].reshape(fresh, -1)
    fresh_values = fresh_v_ref[...].reshape(fresh, -1)

    for index in range(count):
        q_ref = q_refs[index]
        half = 0 if index < halves[0] else 1
        within = index - half * halves[0]
        owner = lax.bitwise_xor(me_ref[0], index)
        slots, masks = [], []
        for j in range(per_owner):
            entry = entry_refs[half][within * (per_owner + 1) + j]
            slot = entry // page_count
            length = lengths_ref[request_ref[owner * slots_here + slot]]
            left = jnp.clip(length - (entry - slot * page_count) * page_len, 0, page_len)
            slots.append(slot)
            masks.append(jnp.broadcast_to(spot_of < left, (rows, twice)))
        tags, scores, values = [], [], []
        for g in range(kv_heads):
            for j in range(per_owner):
                start = pl.multiple_of((g * slots_here + slots[j]) * rows, rows)
                both = pages_refs[half][g, within * per_owner + j]
                product = dot_nt(q_ref[pl.ds(start, rows), :], both)
                scores.append(jnp.where(masks[j], product, MASKED))
                tags.append((g, slots[j]))
                values.append(both)
        if index == 0:
            row = lax.broadcasted_iota(jnp.int32, (rows, twice), 0) % steps
            col = lax.broadcasted_iota(jnp.int32, (rows, twice), 1)
            pad = jnp.zeros((twice - fresh, HEAD_SIZE), jnp.bfloat16)
            for g in range(kv_heads):
                lanes = slice(g * HEAD_SIZE, (g + 1) * HEAD_SIZE)
                keys = jnp.concatenate([fresh_keys[:, lanes], pad], axis=0)
                for slot in range(slots_here):
                    start = (g * slots_here + slot) * rows
                    product = dot_nt(q_ref[start : start + rows, :], keys)
                    ok = (col >= slot * steps) & (col - slot * steps <= row)
                    scores.append(jnp.where(ok, product, MASKED))
                    tags.append((g, slot))
                    values.append(None)
        stacked = jnp.concatenate(scores, axis=0)
        row_max = jnp.maximum(jnp.max(stacked, axis=1, keepdims=True), FLOOR)
        weights = jnp.exp((stacked - row_max) * SCALE)
        totals = jnp.sum(weights, axis=1, keepdims=True)
        paged = kv_heads * per_owner * rows
        shifted = pltpu.roll(weights[:paged], 1, 1).astype(jnp.bfloat16)
        sums = []
        for i, both in enumerate(values):
            place = slice(i * rows, (i + 1) * rows)
            if both is None:
                lanes = slice(tags[i][0] * HEAD_SIZE, (tags[i][0] + 1) * HEAD_SIZE)
                sums.append(
                    dot(weights[place, :fresh].astype(jnp.bfloat16), fresh_values[:, lanes])
                )
            else:
                sums.append(dot(shifted[place], both))
        outs, columns = [], []
        for g in range(kv_heads):
            for slot in range(slots_here):
                found = [
                    (tag[1] == slot, slice(i * rows, (i + 1) * rows), sums[i])
                    for i, tag in enumerate(tags)
                    if tag[0] == g and (tag[1] is slot or not isinstance(tag[1], int))
                ]
                best = functools.reduce(
                    jnp.maximum, [jnp.where(mine, row_max[place], FLOOR) for mine, place, _ in found]
                )
                total = jnp.zeros((rows, 1), jnp.float32)
                summed = jnp.zeros((rows, HEAD_SIZE), jnp.float32)
                for mine, place, part in found:
                    factor = jnp.where(mine, jnp.exp((row_max[place] - best) * SCALE), 0.0)
                    total = total + factor * totals[place]
                    summed = summed + factor * part
                result, lse = finish(total, summed, best)
                outs.append(result)
                columns.append(lse)
        if index == 0:
            for b, value in enumerate(outs):
                own_ref[b * rows : (b + 1) * rows, :] = value
            own_lse_ref[...] = put_lse(columns, rows)
        else:
            out_ref = out_refs[index - 1]
            for b, value in enumerate(outs):
                out_ref[b * rows : (b + 1) * rows, :] = value.astype(jnp.bfloat16)
            out_ref[len(outs) * rows :, :] = split_lse(columns, rows)


def decode_part(halves, me, request, lengths, entries, queries, pages, fresh_keys, fresh_values):
    rows = queries[0].shape[0]
    kv_heads, slots_here = pages[0].shape[0], fresh_keys.shape[0]
    block = rows // (kv_heads * slots_here)
    work = len(queries) * rows * pages[0].shape[1] * pages[0].shape[2] // slots_here
    shapes = [
        jax.ShapeDtypeStruct((rows, HEAD_SIZE), jnp.float32),
        jax.ShapeDtypeStruct((block, LANES), jnp.float32),
    ] + [jax.ShapeDtypeStruct((rows + block, HEAD_SIZE), jnp.bfloat16)] * (len(queries) - 1)
    return pl.pallas_call(
        functools.partial(decode_kernel, halves),
        out_shape=shapes,
        in_specs=[SMEM] * (3 + len(halves)) + [VMEM] * (len(queries) + len(halves) + 2),
        out_specs=[VMEM] * len(shapes),
        compiler_params=pltpu.CompilerParams(vmem_limit_bytes=16 * MIB),
        cost_estimate=pl.CostEstimate(
            flops=work * HEAD_SIZE * 4, bytes_accessed=pages[0].size * 4, transcendentals=work
        ),
        name="decode",
    )(me, request, lengths, *entries, *queries, *pages, fresh_keys, fresh_values)


def combine_kernel(own_ref, own_lse_ref, *refs):
    chunk_refs, out_ref = refs[:-1], refs[-1]
    heads = own_ref.shape[1] // HEAD_SIZE
    width = heads * HEAD_SIZE
    factors = merge_factors(
        [own_lse_ref[:, :heads]] + [join_lse(ref[:, width:], heads) for ref in chunk_refs]
    )
    for h in range(heads):
        lanes = slice(h * HEAD_SIZE, (h + 1) * HEAD_SIZE)
        merged = own_ref[:, lanes] * factors[0][:, h : h + 1]
        for ref, factor in zip(chunk_refs, factors[1:]):
            merged = merged + ref[:, lanes].astype(jnp.float32) * factor[:, h : h + 1]
        out_ref[:, lanes] = merged.astype(jnp.bfloat16)


def decode_combine_kernel(own_ref, own_lse_ref, *refs):
    chunk_refs, out_ref = refs[:-1], refs[-1]
    rows = own_lse_ref.shape[0]
    total_rows = own_ref.shape[0]
    blocks = total_rows // rows
    slots_here, steps = out_ref.shape[0], out_ref.shape[1]
    group = rows // steps
    factors = merge_factors(
        [own_lse_ref[:, :blocks]] + [join_lse(ref[total_rows:, :], blocks) for ref in chunk_refs]
    )
    for b in range(blocks):
        block = slice(b * rows, (b + 1) * rows)
        merged = own_ref[block, :] * factors[0][:, b : b + 1]
        for ref, factor in zip(chunk_refs, factors[1:]):
            merged = merged + ref[block, :].astype(jnp.float32) * factor[:, b : b + 1]
        g, slot = b // slots_here, b % slots_here
        for i in range(group):
            lanes = slice((g * group + i) * HEAD_SIZE, (g * group + i + 1) * HEAD_SIZE)
            out_ref[slot, :, lanes] = merged[i * steps : (i + 1) * steps].astype(jnp.bfloat16)


def combine(body, name, own, own_lse, chunks, shape):
    return pl.pallas_call(
        body,
        out_shape=jax.ShapeDtypeStruct(shape, jnp.bfloat16),
        in_specs=[VMEM] * (2 + len(chunks)),
        out_specs=VMEM,
        compiler_params=pltpu.CompilerParams(vmem_limit_bytes=8 * MIB),
        cost_estimate=pl.CostEstimate(
            flops=own.size * 2 * (1 + len(chunks)), bytes_accessed=own.size * 8, transcendentals=0
        ),
        name=name,
    )(own, own_lse, *chunks)


def lower_kernel(x_hbm, down_hbm, up_hbm, base_hbm, out_ref, up_ref, base_ref, x_ref, down_ref, sem):
    copies = [
        pltpu.make_async_copy(source, target, sem.at[i])
        for i, (source, target) in enumerate(
            [(x_hbm, x_ref), (down_hbm, down_ref), (up_hbm, up_ref), (base_hbm, base_ref)]
        )
    ]
    for copy in copies:
        copy.start()
    for copy in copies[:2]:
        copy.wait()
    x = jnp.concatenate(
        [x_ref[slot].astype(jnp.float32) for slot in range(x_ref.shape[0])], axis=0
    )
    out_ref[...] = dot(x.astype(jnp.bfloat16), down_ref[...])
    for copy in copies[2:]:
        copy.wait()


def lower(x, down, up, base):
    rows = x.shape[0] * x.shape[1]
    return pl.pallas_call(
        lower_kernel,
        out_shape=[
            jax.ShapeDtypeStruct((rows, down.shape[1]), jnp.float32),
            jax.ShapeDtypeStruct(up.shape, up.dtype),
            jax.ShapeDtypeStruct(base.shape, base.dtype),
        ],
        in_specs=[HBM] * 4,
        out_specs=[VMEM] * 3,
        scratch_shapes=[
            pltpu.VMEM(x.shape, x.dtype),
            pltpu.VMEM(down.shape, down.dtype),
            pltpu.SemaphoreType.DMA((4,)),
        ],
        compiler_params=pltpu.CompilerParams(vmem_limit_bytes=8 * MIB),
        cost_estimate=pl.CostEstimate(
            flops=2 * rows * down.size, bytes_accessed=down.size * 4, transcendentals=0
        ),
        name="lower",
    )(x, down, up, base)


def adapter_kernel(
    kv_heads, me_ref, request_ref, adapter_ref, rank_ref, low_ref, other_ref, up_ref, base_ref, out_ref
):
    slots_here, steps = base_ref.shape[0], base_ref.shape[1]
    heads = base_ref.shape[2] // HEAD_SIZE
    group = heads // kv_heads
    shape = low_ref.shape
    row_slot = lax.broadcasted_iota(jnp.int32, shape, 0) // steps
    column = lax.broadcasted_iota(jnp.int32, shape, 1)
    first = jnp.zeros(shape, jnp.int32)
    last = jnp.zeros(shape, jnp.int32)
    for slot in range(slots_here):
        request = request_ref[me_ref[0] * slots_here + slot]
        start = adapter_ref[request] * LARGEST_RANK
        first = jnp.where(row_slot == slot, start, first)
        last = jnp.where(row_slot == slot, start + jnp.minimum(rank_ref[request], LARGEST_RANK), last)
    low = low_ref[...] + other_ref[...]
    kept = jnp.where((column >= first) & (column < last), low, 0.0).astype(jnp.bfloat16)
    raised = dot(kept, up_ref[...])
    blocks = [[None] * slots_here for _ in range(kv_heads)]
    for slot in range(slots_here):
        query = base_ref[slot].astype(jnp.float32) + raised[slot * steps : (slot + 1) * steps]
        for g in range(kv_heads):
            blocks[g][slot] = jnp.concatenate(
                [
                    query[:, (g * group + i) * HEAD_SIZE : (g * group + i + 1) * HEAD_SIZE]
                    for i in range(group)
                ],
                axis=0,
            )
    rows = group * steps
    for g in range(kv_heads):
        for slot in range(slots_here):
            b = g * slots_here + slot
            out_ref[b * rows : (b + 1) * rows, :] = blocks[g][slot].astype(jnp.bfloat16)


def adapter_queries(kv_heads, me, request, adapter, rank, low, other, up, base):
    return pl.pallas_call(
        functools.partial(adapter_kernel, kv_heads),
        out_shape=jax.ShapeDtypeStruct((base.size // HEAD_SIZE, HEAD_SIZE), jnp.bfloat16),
        in_specs=[SMEM] * 4 + [VMEM] * 4,
        out_specs=VMEM,
        compiler_params=pltpu.CompilerParams(vmem_limit_bytes=8 * MIB),
        cost_estimate=pl.CostEstimate(
            flops=2 * low.shape[0] * up.size, bytes_accessed=up.size * 2, transcendentals=0
        ),
        name="adapter",
    )(me, request, adapter, rank, low, other, up, base)


def pin(x):
    return pltpu.with_memory_space_constraint(x, pltpu.HBM)


def exchange(x, axis, offset):
    count = lax.axis_size(axis)
    return lax.ppermute(x, axis, [(i, i ^ offset) for i in range(count)])


def per_device(
    final_block_queries,
    final_block_keys,
    final_block_values,
    prompt_cached_keys,
    prompt_cached_values,
    paged_cache_pool,
    step_slot_queries,
    step_token_keys,
    step_token_values,
    normed_step_inputs,
    adapter_down_maps,
    adapter_up_maps,
    slot_request,
    request_page_table,
    lengths,
    request_adapter,
    request_rank,
):
    seq_count = lax.axis_size("seq")
    tensor_count = lax.axis_size("tensor")
    position = lax.axis_index("seq").astype(jnp.int32)
    me = position.reshape(1)
    offsets = list(range(2, seq_count)) + [1]
    arrived = {o: exchange(final_block_queries, "seq", o) for o in offsets}

    slots_here = step_slot_queries.shape[0]
    kv_heads = final_block_keys.shape[1] // HEAD_SIZE
    request, table, lengths, request_adapter, request_rank = (
        pin(x) for x in (slot_request, request_page_table.T, lengths, request_adapter, request_rank)
    )
    low, up, base = lower(
        pin(normed_step_inputs), pin(adapter_down_maps), pin(adapter_up_maps), pin(step_slot_queries)
    )
    bit, other = 1, jnp.zeros_like(low)
    while bit < tensor_count:
        if bit > 1:
            low = low + other
        other = exchange(low, "tensor", bit)
        bit *= 2
    decode_queries = adapter_queries(
        kv_heads, me, request, request_adapter, request_rank, low, other, up, base
    )
    decode_arrived = {0: decode_queries}
    for o in offsets:
        decode_arrived[o] = exchange(decode_queries, "seq", o)

    load = [
        pin(x)
        for x in (
            prompt_cached_keys, prompt_cached_values, final_block_keys, final_block_values,
            step_token_keys, step_token_values, final_block_queries,
        )
    ]
    halves = (seq_count // 2, seq_count - seq_count // 2)
    pool = pin(paged_cache_pool)
    returned, pages, entries = [], [], []
    for o in offsets:
        allow = ((position ^ o) > position).astype(jnp.int32).reshape(1)
        step = len(returned)
        if step < 2:
            *loaded, part, found, entry = prefill_fetch(
                (step * halves[0], halves[step]), slots_here, allow, arrived[o],
                None if step == 0 else shared, load if step == 0 else [], me, request, table, pool,
            )
            if step == 0:
                shared, fresh, own_queries = loaded[:4], loaded[4:6], loaded[6]
            pages.append(found)
            entries.append(entry)
        else:
            (part,) = prefill_part("far", allow, arrived[o], *shared)
        returned.append(exchange(part, "seq", o))

    parts = decode_part(
        halves, me, request, lengths, entries, [decode_arrived[o] for o in range(seq_count)], pages,
        *fresh,
    )
    decode_returned = [exchange(parts[1 + o], "seq", o) for o in offsets]

    none = jnp.zeros((1,), jnp.int32)
    own, own_lse = prefill_part("own", none, own_queries, *shared)
    prefill_out = combine(combine_kernel, "combine", own, own_lse, returned, own.shape)
    decode_out = combine(
        decode_combine_kernel, "decode_combine", parts[0], parts[1], decode_returned,
        step_slot_queries.shape,
    )
    return (prefill_out, decode_out)


def solution(mesh):
    placed = (
        P(("groups", "seq"), "tensor"),
        P(("groups", "seq"), "tensor"),
        P(("groups", "seq"), "tensor"),
        P(("groups", "seq"), "tensor"),
        P(("groups", "seq"), "tensor"),
        P(("groups", "seq"), None, None, "tensor"),
        P(("groups", "seq"), None, "tensor"),
        P(("groups", "seq"), None, "tensor"),
        P(("groups", "seq"), None, "tensor"),
        P(("groups", "seq"), None, "tensor"),
        P("tensor", None),
        P(None, "tensor"),
        P("groups"),
        P("groups", None),
        P("groups"),
        P("groups"),
        P("groups"),
    )
    return jax.shard_map(
        per_device,
        mesh=mesh,
        in_specs=placed,
        out_specs=(P(("groups", "seq"), "tensor"), P(("groups", "seq"), None, "tensor")),
        check_vma=False,
    )
```

```python
import functools

import jax
import jax.numpy as jnp
from jax import lax
from jax.experimental import pallas as pl
from jax.experimental.pallas import tpu as pltpu
from jax.sharding import PartitionSpec as P

HEAD_SIZE = 128
LARGEST_RANK = 16
LANES = 128
MIB = 1 << 20
MASKED = -1e30
FLOOR = -1e29
SCALE = HEAD_SIZE ** (-0.5)


VMEM = pl.BlockSpec(memory_space=pltpu.VMEM)
SMEM = pl.BlockSpec(memory_space=pltpu.SMEM)
HBM = pl.BlockSpec(memory_space=pltpu.HBM)


def dot_nt(a, b):
    return lax.dot_general(a, b, (((1,), (1,)), ((), ())), preferred_element_type=jnp.float32)


def dot(a, b):
    return jnp.dot(a, b, preferred_element_type=jnp.float32)


def split_three(x):
    high = x.astype(jnp.bfloat16)
    rest = x - high.astype(jnp.float32)
    mid = rest.astype(jnp.bfloat16)
    low = (rest - mid.astype(jnp.float32)).astype(jnp.bfloat16)
    return high, mid, low


def put_lse(columns, rows):
    lane = lax.broadcasted_iota(jnp.int32, (rows, LANES), 1)
    tile = jnp.zeros((rows, LANES), jnp.float32)
    for h, column in enumerate(columns):
        tile = jnp.where(lane == h, column, tile)
    return tile


def split_lse(columns, rows):
    lane = lax.broadcasted_iota(jnp.int32, (rows, LANES), 1)
    count = len(columns)
    whole = put_lse(columns, rows)
    pieces = [piece.astype(jnp.float32) for piece in split_three(whole)]
    tile = pieces[0]
    for index in (1, 2):
        moved = pltpu.roll(pieces[index], index * count, 1)
        tile = jnp.where(lane >= index * count, moved, tile)
    return tile.astype(jnp.bfloat16)


def join_lse(tile, count):
    tile = tile.astype(jnp.float32)
    return tile[:, :count] + tile[:, count : 2 * count] + tile[:, 2 * count : 3 * count]


def merge_factors(lses):
    best = functools.reduce(jnp.maximum, lses)
    factors = [jnp.exp(lse - best) for lse in lses]
    inverse = 1.0 / functools.reduce(jnp.add, factors)
    return [factor * inverse for factor in factors]


def store_remote(out_ref, outs, columns, rows):
    heads = len(outs)
    for h, value in enumerate(outs):
        out_ref[:, h * HEAD_SIZE : (h + 1) * HEAD_SIZE] = value.astype(jnp.bfloat16)
    out_ref[:, heads * HEAD_SIZE :] = split_lse(columns, rows)


def store_own(out_ref, lse_ref, outs, columns, rows):
    for h, value in enumerate(outs):
        out_ref[:, h * HEAD_SIZE : (h + 1) * HEAD_SIZE] = value
    lse_ref[...] = put_lse(columns, rows)


def finish(total, summed, row_max):
    safe = jnp.where(total > 0.0, total, 1.0)
    lse = jnp.where(total > 0.0, row_max * SCALE + jnp.log(safe), MASKED)
    return summed * (1.0 / safe), lse


def load_kernel(load_count, after_ref, *refs):
    del after_ref
    sources, targets, sem = refs[:load_count], refs[load_count:-1], refs[-1]
    pairs = list(zip(sources[:-1], targets[:-1]))
    pool_here = sources[-1].shape[0]
    pieces = 4 if pool_here % 4 == 0 else 1
    for i in range(pieces):
        part = pl.ds(i * (pool_here // pieces), pool_here // pieces)
        pairs.append((sources[-1].at[part], targets[-1].at[part]))
    copies = [
        pltpu.make_async_copy(source, target, sem.at[i]) for i, (source, target) in enumerate(pairs)
    ]
    for copy in copies:
        copy.start()
    for copy in copies:
        copy.wait()


def load_all(after, arrays):
    return pl.pallas_call(
        functools.partial(load_kernel, len(arrays)),
        out_shape=[jax.ShapeDtypeStruct(x.shape, x.dtype) for x in arrays],
        in_specs=[VMEM] + [HBM] * len(arrays),
        out_specs=[VMEM] * len(arrays),
        scratch_shapes=[pltpu.SemaphoreType.DMA((len(arrays) + 3,))],
        compiler_params=pltpu.CompilerParams(vmem_limit_bytes=8 * MIB),
        cost_estimate=pl.CostEstimate(
            flops=10**9, bytes_accessed=2 * sum(x.size for x in arrays), transcendentals=0
        ),
        name="load",
    )(after, *arrays)


def prefill_rows(kind, allow, q_ref, k_ref, v_ref, fresh_k_ref, fresh_v_ref):
    rows = q_ref.shape[0]
    fresh = fresh_k_ref.shape[0]
    kv_heads = k_ref.shape[1] // HEAD_SIZE
    group = q_ref.shape[1] // HEAD_SIZE // kv_heads
    outs, columns = [], []
    for g in range(kv_heads):
        lanes = slice(g * HEAD_SIZE, (g + 1) * HEAD_SIZE)
        query = jnp.concatenate(
            [
                q_ref[:, (g * group + i) * HEAD_SIZE : (g * group + i + 1) * HEAD_SIZE]
                for i in range(group)
            ],
            axis=0,
        )
        scores = dot_nt(query, k_ref[:, lanes])
        fresh_scores = dot_nt(query, fresh_k_ref[:, lanes])
        shape = (group * rows, fresh)
        row = lax.broadcasted_iota(jnp.int32, shape, 0)
        if kind == "own":
            ok = lax.broadcasted_iota(jnp.int32, shape, 1) <= row % rows
        else:
            ok = row < allow * group * rows
        fresh_scores = jnp.where(ok, fresh_scores, MASKED)
        row_max = jnp.maximum(
            jnp.max(scores, axis=1, keepdims=True), jnp.max(fresh_scores, axis=1, keepdims=True)
        )
        weights = jnp.exp((scores - row_max) * SCALE)
        fresh_weights = jnp.where(ok, jnp.exp((fresh_scores - row_max) * SCALE), 0.0)
        total = jnp.sum(weights, axis=1, keepdims=True) + jnp.sum(
            fresh_weights, axis=1, keepdims=True
        )
        summed = dot(weights.astype(jnp.bfloat16), v_ref[:, lanes]) + dot(
            fresh_weights.astype(jnp.bfloat16), fresh_v_ref[:, lanes]
        )
        result, lse = finish(total, summed, row_max)
        for i in range(group):
            outs.append(result[i * rows : (i + 1) * rows])
            columns.append(lse[i * rows : (i + 1) * rows])
    return outs, columns


def prefill_kernel(offset, me_ref, q_ref, k_ref, v_ref, fresh_k_ref, fresh_v_ref, *refs):
    rows = q_ref.shape[0]
    kind = "far" if offset else "own"
    allow = (lax.bitwise_xor(me_ref[0], offset) > me_ref[0]).astype(jnp.int32)
    outs, columns = prefill_rows(
        kind, allow, q_ref, k_ref, v_ref, fresh_k_ref, fresh_v_ref
    )
    if kind == "own":
        store_own(refs[0], refs[1], outs, columns, rows)
    else:
        store_remote(refs[0], outs, columns, rows)


def prefill_cost(queries, keys, fresh_keys):
    work = queries.size // HEAD_SIZE * (keys.shape[0] + fresh_keys.shape[0])
    return pl.CostEstimate(
        flops=work * HEAD_SIZE * 4, bytes_accessed=keys.size * 4, transcendentals=work
    )


def prefill_part(offset, me, queries, keys, values, fresh_keys, fresh_values):
    rows, width = queries.shape
    kind = "far" if offset else "own"
    if kind == "own":
        shapes = [
            jax.ShapeDtypeStruct((rows, width), jnp.float32),
            jax.ShapeDtypeStruct((rows, LANES), jnp.float32),
        ]
    else:
        shapes = [jax.ShapeDtypeStruct((rows, width + LANES), jnp.bfloat16)]
    return pl.pallas_call(
        functools.partial(prefill_kernel, offset),
        out_shape=shapes,
        in_specs=[SMEM] + [VMEM] * 5,
        out_specs=[VMEM] * len(shapes),
        compiler_params=pltpu.CompilerParams(vmem_limit_bytes=16 * MIB),
        cost_estimate=prefill_cost(queries, keys, fresh_keys),
        name="prefill_" + kind,
    )(me, queries, keys, values, fresh_keys, fresh_values)


def decode_kernel(me_ref, request_ref, table_ref, lengths_ref, *refs):
    code_ref, refs = refs[-1], refs[:-1]
    count = (len(refs) - 4) // 2
    q_refs = refs[:count]
    pages_ref, fresh_k_ref, fresh_v_ref = refs[count : count + 3]
    own_ref, own_lse_ref = refs[count + 3 : count + 5]
    out_refs = refs[count + 5 :]
    page_rows = pages_ref.shape[1]
    slots_here, steps = fresh_k_ref.shape[0], fresh_k_ref.shape[1]
    kv_heads = fresh_k_ref.shape[2] // HEAD_SIZE
    page_len = page_rows // (2 * kv_heads)
    page_count = table_ref.shape[0]
    entries = slots_here * page_count
    per_owner = entries // count
    pool_here = pages_ref.shape[0]
    me = me_ref[0]
    rows = q_refs[0].shape[0] // slots_here
    block = rows // kv_heads
    fresh = slots_here * steps
    column = lax.broadcasted_iota(jnp.int32, (rows, page_rows), 1)
    row_head = lax.broadcasted_iota(jnp.int32, (rows, page_rows), 0) // block
    wanted = (column % 2 == 0) & ((column // 2) % kv_heads == row_head)
    spot_of = jnp.where(wanted, column // (2 * kv_heads), page_len)

    def find(index, carry):
        owner = lax.bitwise_xor(me, index)
        found = index * (per_owner + 1)
        last = found + per_owner
        for slot in range(slots_here):
            request = request_ref[owner * slots_here + slot]
            for place in range(page_count):
                local = table_ref[place, request] - me * pool_here
                code_ref[found] = local * entries + slot * page_count + place
                mine = (local >= 0) & (local < pool_here)
                found = jnp.minimum(found + mine.astype(jnp.int32), last)
        return carry

    if count <= 4:
        for index in range(count):
            find(index, 0)
    else:
        lax.fori_loop(0, count, find, 0)

    for index in range(count):
        q_ref = q_refs[index]
        owner = lax.bitwise_xor(me, index)
        slots, scores, pages = [], [], []
        for j in range(per_owner):
            code = code_ref[index * (per_owner + 1) + j]
            local = code // entries
            entry = code - local * entries
            slot = entry // page_count
            length = lengths_ref[request_ref[owner * slots_here + slot]]
            left = jnp.clip(length - (entry - slot * page_count) * page_len, 0, page_len)
            page = pages_ref[local]
            query = q_ref[pl.ds(pl.multiple_of(slot * rows, rows), rows), :]
            scores.append(jnp.where(spot_of < left, dot_nt(query, page), MASKED))
            slots.append(slot)
            pages.append(page)
        stacked = jnp.concatenate(scores, axis=0)
        row_max = jnp.maximum(jnp.max(stacked, axis=1, keepdims=True), FLOOR)
        weights = jnp.exp((stacked - row_max) * SCALE)
        totals = jnp.sum(weights, axis=1, keepdims=True)
        shifted = jnp.concatenate(
            [
                pltpu.roll(weights[:, i * LANES : (i + 1) * LANES], 1, 1).astype(jnp.bfloat16)
                for i in range(page_rows // LANES)
            ],
            axis=1,
        )
        parts = []
        for j in range(per_owner):
            place = slice(j * rows, (j + 1) * rows)
            parts.append((slots[j], row_max[place], totals[place], dot(shifted[place], pages[j])))
        if index == 0:
            fresh_keys = fresh_k_ref[...].reshape(fresh, -1)
            fresh_values = fresh_v_ref[...].reshape(fresh, -1)
            step = lax.broadcasted_iota(jnp.int32, (block, fresh), 0) % steps
            col = lax.broadcasted_iota(jnp.int32, (block, fresh), 1)
            scores = []
            for slot in range(slots_here):
                ok = (col >= slot * steps) & (col - slot * steps <= step)
                for g in range(kv_heads):
                    start = slot * rows + g * block
                    product = dot_nt(
                        q_ref[start : start + block, :],
                        fresh_keys[:, g * HEAD_SIZE : (g + 1) * HEAD_SIZE],
                    )
                    scores.append(jnp.where(ok, product, MASKED))
            stacked = jnp.concatenate(scores, axis=0)
            fresh_max = jnp.max(stacked, axis=1, keepdims=True)
            weights = jnp.exp((stacked - fresh_max) * SCALE)
            fresh_totals = jnp.sum(weights, axis=1, keepdims=True)
            weights = weights.astype(jnp.bfloat16)
            for slot in range(slots_here):
                sums = []
                for g in range(kv_heads):
                    start = slot * rows + g * block
                    sums.append(
                        dot(
                            weights[start : start + block],
                            fresh_values[:, g * HEAD_SIZE : (g + 1) * HEAD_SIZE],
                        )
                    )
                place = slice(slot * rows, (slot + 1) * rows)
                parts.append(
                    (slot, fresh_max[place], fresh_totals[place], jnp.concatenate(sums, axis=0))
                )
        outs, columns = [], []
        for slot in range(slots_here):
            found = [part for part in parts if not isinstance(part[0], int) or part[0] == slot]
            best = functools.reduce(
                jnp.maximum, [jnp.where(part[0] == slot, part[1], FLOOR) for part in found]
            )
            total = jnp.zeros((rows, 1), jnp.float32)
            summed = jnp.zeros((rows, HEAD_SIZE), jnp.float32)
            for part in found:
                factor = jnp.where(part[0] == slot, jnp.exp((part[1] - best) * SCALE), 0.0)
                total = total + factor * part[2]
                summed = summed + factor * part[3]
            result, lse = finish(total, summed, best)
            outs.append(result)
            columns += [lse[g * block : (g + 1) * block] for g in range(kv_heads)]
        if index == 0:
            for slot, value in enumerate(outs):
                own_ref[slot * rows : (slot + 1) * rows, :] = value
            own_lse_ref[...] = put_lse(columns, block)
        else:
            out_ref = out_refs[index - 1]
            for slot, value in enumerate(outs):
                out_ref[slot * rows : (slot + 1) * rows, :] = value.astype(jnp.bfloat16)
            out_ref[slots_here * rows :, :] = split_lse(columns, block)


def decode_part(me, request, table, lengths, queries, pages, fresh_keys, fresh_values):
    rows = queries[0].shape[0]
    block = rows // (fresh_keys.shape[0] * fresh_keys.shape[2] // HEAD_SIZE)
    work = pages.shape[0] * pages.shape[1] * rows // fresh_keys.shape[0]
    shapes = [
        jax.ShapeDtypeStruct((rows, HEAD_SIZE), jnp.float32),
        jax.ShapeDtypeStruct((block, LANES), jnp.float32),
    ] + [jax.ShapeDtypeStruct((rows + block, HEAD_SIZE), jnp.bfloat16)] * (len(queries) - 1)
    return pl.pallas_call(
        decode_kernel,
        out_shape=shapes,
        in_specs=[SMEM] * 4 + [VMEM] * (len(queries) + 3),
        out_specs=[VMEM] * len(shapes),
        scratch_shapes=[pltpu.SMEM((table.size // request.shape[0] * fresh_keys.shape[0] + len(queries),), jnp.int32)],
        compiler_params=pltpu.CompilerParams(vmem_limit_bytes=16 * MIB),
        cost_estimate=pl.CostEstimate(
            flops=work * HEAD_SIZE * 4, bytes_accessed=pages.size * 2, transcendentals=work
        ),
        name="decode",
    )(me, request, table, lengths, *queries, pages, fresh_keys, fresh_values)


def combine_kernel(count, own_ref, own_lse_ref, *refs):
    chunk_refs, out_ref = refs[:count], refs[-1]
    heads = own_ref.shape[1] // HEAD_SIZE
    width = heads * HEAD_SIZE
    factors = merge_factors(
        [own_lse_ref[:, :heads]] + [join_lse(ref[:, width:], heads) for ref in chunk_refs]
    )
    for h in range(heads):
        lanes = slice(h * HEAD_SIZE, (h + 1) * HEAD_SIZE)
        merged = own_ref[:, lanes] * factors[0][:, h : h + 1]
        for ref, factor in zip(chunk_refs, factors[1:]):
            merged = merged + ref[:, lanes].astype(jnp.float32) * factor[:, h : h + 1]
        out_ref[:, lanes] = merged.astype(jnp.bfloat16)


def decode_combine_kernel(count, own_ref, own_lse_ref, *refs):
    chunk_refs, out_ref = refs[:count], refs[-1]
    rows = own_lse_ref.shape[0]
    total_rows = own_ref.shape[0]
    blocks = total_rows // rows
    steps = out_ref.shape[1]
    kv_heads = blocks // out_ref.shape[0]
    group = rows // steps
    factors = merge_factors(
        [own_lse_ref[:, :blocks]] + [join_lse(ref[total_rows:, :], blocks) for ref in chunk_refs]
    )
    for b in range(blocks):
        block = slice(b * rows, (b + 1) * rows)
        merged = own_ref[block, :] * factors[0][:, b : b + 1]
        for ref, factor in zip(chunk_refs, factors[1:]):
            merged = merged + ref[block, :].astype(jnp.float32) * factor[:, b : b + 1]
        g, slot = b % kv_heads, b // kv_heads
        for i in range(group):
            lanes = slice((g * group + i) * HEAD_SIZE, (g * group + i + 1) * HEAD_SIZE)
            out_ref[slot, :, lanes] = merged[i * steps : (i + 1) * steps].astype(jnp.bfloat16)


def combine(body, name, own, own_lse, chunks, shape, after=None):
    extra = [] if after is None else [after]
    return pl.pallas_call(
        functools.partial(body, len(chunks)),
        out_shape=jax.ShapeDtypeStruct(shape, jnp.bfloat16),
        in_specs=[VMEM] * (2 + len(chunks)) + [HBM] * len(extra),
        out_specs=VMEM,
        compiler_params=pltpu.CompilerParams(vmem_limit_bytes=8 * MIB),
        cost_estimate=pl.CostEstimate(
            flops=own.size * 2 * (1 + len(chunks)), bytes_accessed=own.size * 8, transcendentals=0
        ),
        name=name,
    )(own, own_lse, *chunks, *extra)


def lower_kernel(x_hbm, down_hbm, up_hbm, base_hbm, out_ref, up_ref, base_ref, x_ref, down_ref, sem):
    copies = [
        pltpu.make_async_copy(source, target, sem.at[i])
        for i, (source, target) in enumerate(
            [(x_hbm, x_ref), (down_hbm, down_ref), (up_hbm, up_ref), (base_hbm, base_ref)]
        )
    ]
    for copy in copies:
        copy.start()
    for copy in copies[:2]:
        copy.wait()
    x = jnp.concatenate(
        [x_ref[slot].astype(jnp.float32) for slot in range(x_ref.shape[0])], axis=0
    )
    out_ref[...] = dot(x.astype(jnp.bfloat16), down_ref[...])
    for copy in copies[2:]:
        copy.wait()


def lower(x, down, up, base):
    rows = x.shape[0] * x.shape[1]
    return pl.pallas_call(
        lower_kernel,
        out_shape=[
            jax.ShapeDtypeStruct((rows, down.shape[1]), jnp.float32),
            jax.ShapeDtypeStruct(up.shape, up.dtype),
            jax.ShapeDtypeStruct(base.shape, base.dtype),
        ],
        in_specs=[HBM] * 4,
        out_specs=[VMEM] * 3,
        scratch_shapes=[
            pltpu.VMEM(x.shape, x.dtype),
            pltpu.VMEM(down.shape, down.dtype),
            pltpu.SemaphoreType.DMA((4,)),
        ],
        compiler_params=pltpu.CompilerParams(vmem_limit_bytes=8 * MIB),
        cost_estimate=pl.CostEstimate(
            flops=2 * rows * down.size, bytes_accessed=down.size * 4, transcendentals=0
        ),
        name="lower",
    )(x, down, up, base)


def adapter_kernel(
    kv_heads, me_ref, request_ref, adapter_ref, rank_ref, low_ref, other_ref, up_ref, base_ref,
    after_ref, out_ref
):
    del after_ref
    slots_here, steps = base_ref.shape[0], base_ref.shape[1]
    heads = base_ref.shape[2] // HEAD_SIZE
    group = heads // kv_heads
    shape = low_ref.shape
    row_slot = lax.broadcasted_iota(jnp.int32, shape, 0) // steps
    column = lax.broadcasted_iota(jnp.int32, shape, 1)
    first = jnp.zeros(shape, jnp.int32)
    last = jnp.zeros(shape, jnp.int32)
    for slot in range(slots_here):
        request = request_ref[me_ref[0] * slots_here + slot]
        start = adapter_ref[request] * LARGEST_RANK
        first = jnp.where(row_slot == slot, start, first)
        last = jnp.where(row_slot == slot, start + jnp.minimum(rank_ref[request], LARGEST_RANK), last)
    low = low_ref[...] + other_ref[...]
    kept = jnp.where((column >= first) & (column < last), low, 0.0).astype(jnp.bfloat16)
    raised = dot(kept, up_ref[...])
    blocks = [[None] * slots_here for _ in range(kv_heads)]
    for slot in range(slots_here):
        query = base_ref[slot].astype(jnp.float32) + raised[slot * steps : (slot + 1) * steps]
        for g in range(kv_heads):
            blocks[g][slot] = jnp.concatenate(
                [
                    query[:, (g * group + i) * HEAD_SIZE : (g * group + i + 1) * HEAD_SIZE]
                    for i in range(group)
                ],
                axis=0,
            )
    rows = group * steps
    for g in range(kv_heads):
        for slot in range(slots_here):
            b = slot * kv_heads + g
            out_ref[b * rows : (b + 1) * rows, :] = blocks[g][slot].astype(jnp.bfloat16)


def adapter_queries(kv_heads, me, request, adapter, rank, low, other, up, base, after):
    return pl.pallas_call(
        functools.partial(adapter_kernel, kv_heads),
        out_shape=jax.ShapeDtypeStruct((base.size // HEAD_SIZE, HEAD_SIZE), jnp.bfloat16),
        in_specs=[SMEM] * 4 + [VMEM] * 5,
        out_specs=VMEM,
        compiler_params=pltpu.CompilerParams(vmem_limit_bytes=8 * MIB),
        cost_estimate=pl.CostEstimate(
            flops=2 * low.shape[0] * up.size, bytes_accessed=up.size * 2, transcendentals=0
        ),
        name="adapter",
    )(me, request, adapter, rank, low, other, up, base, after)


def pin(x):
    return pltpu.with_memory_space_constraint(x, pltpu.HBM)


def exchange(x, axis, offset):
    count = lax.axis_size(axis)
    return lax.ppermute(x, axis, [(i, i ^ offset) for i in range(count)])


def gather(held, axis, bit):
    while bit:
        for offset in list(held):
            held[offset | bit] = exchange(held[offset], axis, bit)
        bit //= 2
    return held


def per_device(
    final_block_queries,
    final_block_keys,
    final_block_values,
    prompt_cached_keys,
    prompt_cached_values,
    paged_cache_pool,
    step_slot_queries,
    step_token_keys,
    step_token_values,
    normed_step_inputs,
    adapter_down_maps,
    adapter_up_maps,
    slot_request,
    request_page_table,
    lengths,
    request_adapter,
    request_rank,
):
    seq_count = lax.axis_size("seq")
    tensor_count = lax.axis_size("tensor")
    position = lax.axis_index("seq").astype(jnp.int32)
    me = position.reshape(1)
    offsets = list(range(2, seq_count)) + [1]
    half = seq_count // 2
    arrived = {half: exchange(final_block_queries, "seq", half)}

    slots_here = step_slot_queries.shape[0]
    kv_heads = final_block_keys.shape[1] // HEAD_SIZE
    request, table, lengths, request_adapter, request_rank = (
        pin(x) for x in (slot_request, request_page_table.T, lengths, request_adapter, request_rank)
    )
    low, up, base = lower(
        pin(normed_step_inputs), pin(adapter_down_maps), pin(adapter_up_maps), pin(step_slot_queries)
    )
    bit, other = 1, jnp.zeros_like(low)
    while bit < tensor_count:
        if bit > 1:
            low = low + other
        other = exchange(low, "tensor", bit)
        bit *= 2
    load = [
        pin(x)
        for x in (
            prompt_cached_keys, prompt_cached_values, final_block_keys, final_block_values,
            step_token_keys, step_token_values, final_block_queries,
        )
    ]
    pool = paged_cache_pool.reshape(*paged_cache_pool.shape[:3], kv_heads, HEAD_SIZE)
    pool = pin(pool.transpose(0, 1, 3, 2, 4))
    *loaded, pages = load_all(low, load + [pool])
    pages = pages.reshape(pages.shape[0], -1, HEAD_SIZE)
    shared, fresh, own_queries = loaded[:4], loaded[4:6], loaded[6]
    decode_queries = adapter_queries(
        kv_heads, me, request, request_adapter, request_rank, low, other, up, base, fresh[0]
    )
    arrived[half], decode_queries = lax.optimization_barrier((arrived[half], decode_queries))
    arrived = gather({0: final_block_queries} | arrived, "seq", half // 2)
    decode_arrived = {0: decode_queries}
    for o in offsets:
        decode_arrived[o] = exchange(decode_queries, "seq", o)
    returned = []
    for o in offsets:
        (part,) = prefill_part(o, me, arrived[o], *shared)
        returned.append(exchange(part, "seq", o))

    parts = decode_part(
        me, request, table, lengths, [decode_arrived[o] for o in range(seq_count)], pages, *fresh
    )
    decode_returned = [exchange(parts[1 + o], "seq", o) for o in offsets]

    own, own_lse = prefill_part(0, me, own_queries, *shared)
    prefill_out = combine(combine_kernel, "combine", own, own_lse, returned, own.shape)
    decode_out = combine(
        decode_combine_kernel, "decode_combine", parts[0], parts[1], decode_returned,
        step_slot_queries.shape, pin(prefill_out),
    )
    return (prefill_out, decode_out)


def solution(mesh):
    placed = (
        P(("groups", "seq"), "tensor"),
        P(("groups", "seq"), "tensor"),
        P(("groups", "seq"), "tensor"),
        P(("groups", "seq"), "tensor"),
        P(("groups", "seq"), "tensor"),
        P(("groups", "seq"), None, None, "tensor"),
        P(("groups", "seq"), None, "tensor"),
        P(("groups", "seq"), None, "tensor"),
        P(("groups", "seq"), None, "tensor"),
        P(("groups", "seq"), None, "tensor"),
        P("tensor", None),
        P(None, "tensor"),
        P("groups"),
        P("groups", None),
        P("groups"),
        P("groups"),
        P("groups"),
    )
    return jax.shard_map(
        per_device,
        mesh=mesh,
        in_specs=placed,
        out_specs=(P(("groups", "seq"), "tensor"), P(("groups", "seq"), None, "tensor")),
        check_vma=False,
    )
```

```python
import functools

import jax
import jax.numpy as jnp
from jax import lax
from jax.experimental import pallas as pl
from jax.experimental.pallas import tpu as pltpu
from jax.sharding import PartitionSpec as P

HEAD_SIZE = 128
LARGEST_RANK = 16
LANES = 128
MIB = 1 << 20
MASKED = -1e30
FLOOR = -1e29
SCALE = HEAD_SIZE ** (-0.5)


VMEM = pl.BlockSpec(memory_space=pltpu.VMEM)
SMEM = pl.BlockSpec(memory_space=pltpu.SMEM)
HBM = pl.BlockSpec(memory_space=pltpu.HBM)


def dot_nt(a, b):
    return lax.dot_general(a, b, (((1,), (1,)), ((), ())), preferred_element_type=jnp.float32)


def dot(a, b):
    return jnp.dot(a, b, preferred_element_type=jnp.float32)


def split_three(x):
    high = x.astype(jnp.bfloat16)
    rest = x - high.astype(jnp.float32)
    mid = rest.astype(jnp.bfloat16)
    low = (rest - mid.astype(jnp.float32)).astype(jnp.bfloat16)
    return high, mid, low


def put_lse(columns, rows):
    lane = lax.broadcasted_iota(jnp.int32, (rows, LANES), 1)
    tile = jnp.zeros((rows, LANES), jnp.float32)
    for h, column in enumerate(columns):
        tile = jnp.where(lane == h, column, tile)
    return tile


def split_lse(columns, rows):
    lane = lax.broadcasted_iota(jnp.int32, (rows, LANES), 1)
    count = len(columns)
    whole = put_lse(columns, rows)
    pieces = [piece.astype(jnp.float32) for piece in split_three(whole)]
    tile = pieces[0]
    for index in (1, 2):
        moved = pltpu.roll(pieces[index], index * count, 1)
        tile = jnp.where(lane >= index * count, moved, tile)
    return tile.astype(jnp.bfloat16)


def join_lse(tile, count):
    tile = tile.astype(jnp.float32)
    return tile[:, :count] + tile[:, count : 2 * count] + tile[:, 2 * count : 3 * count]


def merge_factors(lses):
    best = functools.reduce(jnp.maximum, lses)
    factors = [jnp.exp(lse - best) for lse in lses]
    inverse = 1.0 / functools.reduce(jnp.add, factors)
    return [factor * inverse for factor in factors]


def store_remote(out_ref, outs, columns, rows):
    heads = len(outs)
    for h, value in enumerate(outs):
        out_ref[:, h * HEAD_SIZE : (h + 1) * HEAD_SIZE] = value.astype(jnp.bfloat16)
    out_ref[:, heads * HEAD_SIZE :] = split_lse(columns, rows)


def store_own(out_ref, lse_ref, outs, columns, rows):
    for h, value in enumerate(outs):
        out_ref[:, h * HEAD_SIZE : (h + 1) * HEAD_SIZE] = value
    lse_ref[...] = put_lse(columns, rows)


def finish(total, summed, row_max):
    safe = jnp.where(total > 0.0, total, 1.0)
    lse = jnp.where(total > 0.0, row_max * SCALE + jnp.log(safe), MASKED)
    return summed * (1.0 / safe), lse


def load_kernel(load_count, after_ref, *refs):
    del after_ref
    sources, targets, sem = refs[:load_count], refs[load_count:-1], refs[-1]
    pairs = list(zip(sources[:-1], targets[:-1]))
    pool_here = sources[-1].shape[0]
    pieces = 4 if pool_here % 4 == 0 else 1
    for i in range(pieces):
        part = pl.ds(i * (pool_here // pieces), pool_here // pieces)
        pairs.append((sources[-1].at[part], targets[-1].at[part]))
    copies = [
        pltpu.make_async_copy(source, target, sem.at[i]) for i, (source, target) in enumerate(pairs)
    ]
    for copy in copies:
        copy.start()
    for copy in copies:
        copy.wait()


def load_all(after, arrays):
    return pl.pallas_call(
        functools.partial(load_kernel, len(arrays)),
        out_shape=[jax.ShapeDtypeStruct(x.shape, x.dtype) for x in arrays],
        in_specs=[VMEM] + [HBM] * len(arrays),
        out_specs=[VMEM] * len(arrays),
        scratch_shapes=[pltpu.SemaphoreType.DMA((len(arrays) + 3,))],
        compiler_params=pltpu.CompilerParams(vmem_limit_bytes=8 * MIB),
        cost_estimate=pl.CostEstimate(
            flops=10**9, bytes_accessed=2 * sum(x.size for x in arrays), transcendentals=0
        ),
        name="load",
    )(after, *arrays)


def prefill_rows(kind, allow, q_ref, k_ref, v_ref, fresh_k_ref, fresh_v_ref):
    rows = q_ref.shape[0]
    fresh = fresh_k_ref.shape[0]
    kv_heads = k_ref.shape[1] // HEAD_SIZE
    group = q_ref.shape[1] // HEAD_SIZE // kv_heads
    outs, columns = [], []
    for g in range(kv_heads):
        lanes = slice(g * HEAD_SIZE, (g + 1) * HEAD_SIZE)
        query = jnp.concatenate(
            [
                q_ref[:, (g * group + i) * HEAD_SIZE : (g * group + i + 1) * HEAD_SIZE]
                for i in range(group)
            ],
            axis=0,
        )
        scores = dot_nt(query, k_ref[:, lanes])
        fresh_scores = dot_nt(query, fresh_k_ref[:, lanes])
        shape = (group * rows, fresh)
        row = lax.broadcasted_iota(jnp.int32, shape, 0)
        if kind == "own":
            ok = lax.broadcasted_iota(jnp.int32, shape, 1) <= row % rows
        else:
            ok = row < allow * group * rows
        fresh_scores = jnp.where(ok, fresh_scores, MASKED)
        row_max = jnp.maximum(
            jnp.max(scores, axis=1, keepdims=True), jnp.max(fresh_scores, axis=1, keepdims=True)
        )
        weights = jnp.exp((scores - row_max) * SCALE)
        fresh_weights = jnp.where(ok, jnp.exp((fresh_scores - row_max) * SCALE), 0.0)
        total = jnp.sum(weights, axis=1, keepdims=True) + jnp.sum(
            fresh_weights, axis=1, keepdims=True
        )
        summed = dot(weights.astype(jnp.bfloat16), v_ref[:, lanes]) + dot(
            fresh_weights.astype(jnp.bfloat16), fresh_v_ref[:, lanes]
        )
        result, lse = finish(total, summed, row_max)
        for i in range(group):
            outs.append(result[i * rows : (i + 1) * rows])
            columns.append(lse[i * rows : (i + 1) * rows])
    return outs, columns


def merge_chunks(own, own_lse, chunk_refs, out_ref):
    heads = len(own)
    width = heads * HEAD_SIZE
    factors = merge_factors(
        [own_lse[:, :heads]] + [join_lse(ref[:, width:], heads) for ref in chunk_refs]
    )
    for h in range(heads):
        lanes = slice(h * HEAD_SIZE, (h + 1) * HEAD_SIZE)
        merged = own[h] * factors[0][:, h : h + 1]
        for ref, factor in zip(chunk_refs, factors[1:]):
            merged = merged + ref[:, lanes].astype(jnp.float32) * factor[:, h : h + 1]
        out_ref[:, lanes] = merged.astype(jnp.bfloat16)


def prefill_end_kernel(q_ref, k_ref, v_ref, fresh_k_ref, fresh_v_ref, *refs):
    chunk_refs, out_ref = refs[:-1], refs[-1]
    outs, columns = prefill_rows("own", 1, q_ref, k_ref, v_ref, fresh_k_ref, fresh_v_ref)
    merge_chunks(outs, put_lse(columns, q_ref.shape[0]), chunk_refs, out_ref)


def prefill_end(queries, keys, values, fresh_keys, fresh_values, chunks):
    return pl.pallas_call(
        prefill_end_kernel,
        out_shape=jax.ShapeDtypeStruct(queries.shape, jnp.bfloat16),
        in_specs=[VMEM] * (5 + len(chunks)),
        out_specs=VMEM,
        compiler_params=pltpu.CompilerParams(vmem_limit_bytes=16 * MIB),
        cost_estimate=prefill_cost(queries, keys, fresh_keys),
        name="prefill_end",
    )(queries, keys, values, fresh_keys, fresh_values, *chunks)


def prefill_kernel(offset, me_ref, q_ref, k_ref, v_ref, fresh_k_ref, fresh_v_ref, *refs):
    rows = q_ref.shape[0]
    kind = "far" if offset else "own"
    allow = (lax.bitwise_xor(me_ref[0], offset) > me_ref[0]).astype(jnp.int32)
    outs, columns = prefill_rows(
        kind, allow, q_ref, k_ref, v_ref, fresh_k_ref, fresh_v_ref
    )
    if kind == "own":
        store_own(refs[0], refs[1], outs, columns, rows)
    else:
        store_remote(refs[0], outs, columns, rows)


def prefill_cost(queries, keys, fresh_keys):
    work = queries.size // HEAD_SIZE * (keys.shape[0] + fresh_keys.shape[0])
    return pl.CostEstimate(
        flops=work * HEAD_SIZE * 4, bytes_accessed=keys.size * 4, transcendentals=work
    )


def prefill_part(offset, me, queries, keys, values, fresh_keys, fresh_values):
    rows, width = queries.shape
    kind = "far" if offset else "own"
    if kind == "own":
        shapes = [
            jax.ShapeDtypeStruct((rows, width), jnp.float32),
            jax.ShapeDtypeStruct((rows, LANES), jnp.float32),
        ]
    else:
        shapes = [jax.ShapeDtypeStruct((rows, width + LANES), jnp.bfloat16)]
    return pl.pallas_call(
        functools.partial(prefill_kernel, offset),
        out_shape=shapes,
        in_specs=[SMEM] + [VMEM] * 5,
        out_specs=[VMEM] * len(shapes),
        compiler_params=pltpu.CompilerParams(vmem_limit_bytes=16 * MIB),
        cost_estimate=prefill_cost(queries, keys, fresh_keys),
        name="prefill_" + kind,
    )(me, queries, keys, values, fresh_keys, fresh_values)


def decode_kernel(me_ref, request_ref, table_ref, lengths_ref, *refs):
    code_ref, refs = refs[-1], refs[:-1]
    count = (len(refs) - 4) // 2
    q_refs = refs[:count]
    pages_ref, fresh_k_ref, fresh_v_ref = refs[count : count + 3]
    own_ref, own_lse_ref = refs[count + 3 : count + 5]
    out_refs = refs[count + 5 :]
    page_rows = pages_ref.shape[1]
    slots_here, steps = fresh_k_ref.shape[0], fresh_k_ref.shape[1]
    kv_heads = fresh_k_ref.shape[2] // HEAD_SIZE
    page_len = page_rows // (2 * kv_heads)
    page_count = table_ref.shape[0]
    entries = slots_here * page_count
    per_owner = entries // count
    pool_here = pages_ref.shape[0]
    me = me_ref[0]
    rows = q_refs[0].shape[0] // slots_here
    block = rows // kv_heads
    fresh = slots_here * steps
    column = lax.broadcasted_iota(jnp.int32, (rows, page_rows), 1)
    row_head = lax.broadcasted_iota(jnp.int32, (rows, page_rows), 0) // block
    wanted = (column % 2 == 0) & ((column // 2) % kv_heads == row_head)
    spot_of = jnp.where(wanted, column // (2 * kv_heads), page_len)

    def find(index, carry):
        owner = lax.bitwise_xor(me, index)
        found = index * (per_owner + 1)
        last = found + per_owner
        for slot in range(slots_here):
            request = request_ref[owner * slots_here + slot]
            for place in range(page_count):
                local = table_ref[place, request] - me * pool_here
                code_ref[found] = local * entries + slot * page_count + place
                mine = (local >= 0) & (local < pool_here)
                found = jnp.minimum(found + mine.astype(jnp.int32), last)
        return carry

    if count <= 4:
        find(0, 0)
    else:
        lax.fori_loop(0, count, find, 0)

    for index in range(count):
        if count <= 4 and index + 1 < count:
            find(index + 1, 0)
        q_ref = q_refs[index]
        owner = lax.bitwise_xor(me, index)
        slots, scores, pages = [], [], []
        for j in range(per_owner):
            code = code_ref[index * (per_owner + 1) + j]
            local = code // entries
            entry = code - local * entries
            slot = entry // page_count
            length = lengths_ref[request_ref[owner * slots_here + slot]]
            left = jnp.clip(length - (entry - slot * page_count) * page_len, 0, page_len)
            page = pages_ref[local]
            query = q_ref[pl.ds(pl.multiple_of(slot * rows, rows), rows), :]
            scores.append(jnp.where(spot_of < left, dot_nt(query, page), MASKED))
            slots.append(slot)
            pages.append(page)
        stacked = jnp.concatenate(scores, axis=0)
        row_max = jnp.maximum(jnp.max(stacked, axis=1, keepdims=True), FLOOR)
        weights = jnp.exp((stacked - row_max) * SCALE)
        totals = jnp.sum(weights, axis=1, keepdims=True)
        shifted = jnp.concatenate(
            [
                pltpu.roll(weights[:, i * LANES : (i + 1) * LANES], 1, 1).astype(jnp.bfloat16)
                for i in range(page_rows // LANES)
            ],
            axis=1,
        )
        parts = []
        for j in range(per_owner):
            place = slice(j * rows, (j + 1) * rows)
            parts.append((slots[j], row_max[place], totals[place], dot(shifted[place], pages[j])))
        if index == 0:
            fresh_keys = fresh_k_ref[...].reshape(fresh, -1)
            fresh_values = fresh_v_ref[...].reshape(fresh, -1)
            step = lax.broadcasted_iota(jnp.int32, (block, fresh), 0) % steps
            col = lax.broadcasted_iota(jnp.int32, (block, fresh), 1)
            scores = []
            for slot in range(slots_here):
                ok = (col >= slot * steps) & (col - slot * steps <= step)
                for g in range(kv_heads):
                    start = slot * rows + g * block
                    product = dot_nt(
                        q_ref[start : start + block, :],
                        fresh_keys[:, g * HEAD_SIZE : (g + 1) * HEAD_SIZE],
                    )
                    scores.append(jnp.where(ok, product, MASKED))
            stacked = jnp.concatenate(scores, axis=0)
            fresh_max = jnp.max(stacked, axis=1, keepdims=True)
            weights = jnp.exp((stacked - fresh_max) * SCALE)
            fresh_totals = jnp.sum(weights, axis=1, keepdims=True)
            weights = weights.astype(jnp.bfloat16)
            for slot in range(slots_here):
                sums = []
                for g in range(kv_heads):
                    start = slot * rows + g * block
                    sums.append(
                        dot(
                            weights[start : start + block],
                            fresh_values[:, g * HEAD_SIZE : (g + 1) * HEAD_SIZE],
                        )
                    )
                place = slice(slot * rows, (slot + 1) * rows)
                parts.append(
                    (slot, fresh_max[place], fresh_totals[place], jnp.concatenate(sums, axis=0))
                )
        outs, columns = [], []
        for slot in range(slots_here):
            found = [part for part in parts if not isinstance(part[0], int) or part[0] == slot]
            best = functools.reduce(
                jnp.maximum, [jnp.where(part[0] == slot, part[1], FLOOR) for part in found]
            )
            total = jnp.zeros((rows, 1), jnp.float32)
            summed = jnp.zeros((rows, HEAD_SIZE), jnp.float32)
            for part in found:
                factor = jnp.where(part[0] == slot, jnp.exp((part[1] - best) * SCALE), 0.0)
                total = total + factor * part[2]
                summed = summed + factor * part[3]
            result, lse = finish(total, summed, best)
            outs.append(result)
            columns += [lse[g * block : (g + 1) * block] for g in range(kv_heads)]
        if index == 0:
            for slot, value in enumerate(outs):
                own_ref[slot * rows : (slot + 1) * rows, :] = value
            own_lse_ref[...] = put_lse(columns, block)
        else:
            out_ref = out_refs[index - 1]
            for slot, value in enumerate(outs):
                out_ref[slot * rows : (slot + 1) * rows, :] = value.astype(jnp.bfloat16)
            out_ref[slots_here * rows :, :] = split_lse(columns, block)


def decode_part(me, request, table, lengths, queries, pages, fresh_keys, fresh_values):
    rows = queries[0].shape[0]
    block = rows // (fresh_keys.shape[0] * fresh_keys.shape[2] // HEAD_SIZE)
    work = pages.shape[0] * pages.shape[1] * rows // fresh_keys.shape[0]
    shapes = [
        jax.ShapeDtypeStruct((rows, HEAD_SIZE), jnp.float32),
        jax.ShapeDtypeStruct((block, LANES), jnp.float32),
    ] + [jax.ShapeDtypeStruct((rows + block, HEAD_SIZE), jnp.bfloat16)] * (len(queries) - 1)
    return pl.pallas_call(
        decode_kernel,
        out_shape=shapes,
        in_specs=[SMEM] * 4 + [VMEM] * (len(queries) + 3),
        out_specs=[VMEM] * len(shapes),
        scratch_shapes=[pltpu.SMEM((table.size // request.shape[0] * fresh_keys.shape[0] + len(queries),), jnp.int32)],
        compiler_params=pltpu.CompilerParams(vmem_limit_bytes=16 * MIB),
        cost_estimate=pl.CostEstimate(
            flops=work * HEAD_SIZE * 4, bytes_accessed=pages.size * 2, transcendentals=work
        ),
        name="decode",
    )(me, request, table, lengths, *queries, pages, fresh_keys, fresh_values)


def decode_combine_kernel(count, own_ref, own_lse_ref, *refs):
    chunk_refs, out_ref = refs[:count], refs[-1]
    rows = own_lse_ref.shape[0]
    total_rows = own_ref.shape[0]
    blocks = total_rows // rows
    steps = out_ref.shape[1]
    kv_heads = blocks // out_ref.shape[0]
    group = rows // steps
    factors = merge_factors(
        [own_lse_ref[:, :blocks]] + [join_lse(ref[total_rows:, :], blocks) for ref in chunk_refs]
    )
    for b in range(blocks):
        block = slice(b * rows, (b + 1) * rows)
        merged = own_ref[block, :] * factors[0][:, b : b + 1]
        for ref, factor in zip(chunk_refs, factors[1:]):
            merged = merged + ref[block, :].astype(jnp.float32) * factor[:, b : b + 1]
        g, slot = b % kv_heads, b // kv_heads
        for i in range(group):
            lanes = slice((g * group + i) * HEAD_SIZE, (g * group + i + 1) * HEAD_SIZE)
            out_ref[slot, :, lanes] = merged[i * steps : (i + 1) * steps].astype(jnp.bfloat16)


def combine(body, name, own, own_lse, chunks, shape, after=None):
    extra = [] if after is None else [after]
    return pl.pallas_call(
        functools.partial(body, len(chunks)),
        out_shape=jax.ShapeDtypeStruct(shape, jnp.bfloat16),
        in_specs=[VMEM] * (2 + len(chunks)) + [HBM] * len(extra),
        out_specs=VMEM,
        compiler_params=pltpu.CompilerParams(vmem_limit_bytes=8 * MIB),
        cost_estimate=pl.CostEstimate(
            flops=own.size * 2 * (1 + len(chunks)), bytes_accessed=own.size * 8, transcendentals=0
        ),
        name=name,
    )(own, own_lse, *chunks, *extra)


def lower_kernel(x_hbm, down_hbm, up_hbm, base_hbm, out_ref, up_ref, base_ref, x_ref, down_ref, sem):
    copies = [
        pltpu.make_async_copy(source, target, sem.at[i])
        for i, (source, target) in enumerate(
            [(x_hbm, x_ref), (down_hbm, down_ref), (up_hbm, up_ref), (base_hbm, base_ref)]
        )
    ]
    for copy in copies:
        copy.start()
    for copy in copies[:2]:
        copy.wait()
    x = jnp.concatenate(
        [x_ref[slot].astype(jnp.float32) for slot in range(x_ref.shape[0])], axis=0
    )
    out_ref[...] = dot(x.astype(jnp.bfloat16), down_ref[...])
    for copy in copies[2:]:
        copy.wait()


def lower(x, down, up, base):
    rows = x.shape[0] * x.shape[1]
    return pl.pallas_call(
        lower_kernel,
        out_shape=[
            jax.ShapeDtypeStruct((rows, down.shape[1]), jnp.float32),
            jax.ShapeDtypeStruct(up.shape, up.dtype),
            jax.ShapeDtypeStruct(base.shape, base.dtype),
        ],
        in_specs=[HBM] * 4,
        out_specs=[VMEM] * 3,
        scratch_shapes=[
            pltpu.VMEM(x.shape, x.dtype),
            pltpu.VMEM(down.shape, down.dtype),
            pltpu.SemaphoreType.DMA((4,)),
        ],
        compiler_params=pltpu.CompilerParams(vmem_limit_bytes=8 * MIB),
        cost_estimate=pl.CostEstimate(
            flops=2 * rows * down.size, bytes_accessed=down.size * 4, transcendentals=0
        ),
        name="lower",
    )(x, down, up, base)


def adapter_kernel(
    kv_heads, me_ref, request_ref, adapter_ref, rank_ref, low_ref, other_ref, up_ref, base_ref,
    after_ref, out_ref
):
    del after_ref
    slots_here, steps = base_ref.shape[0], base_ref.shape[1]
    heads = base_ref.shape[2] // HEAD_SIZE
    group = heads // kv_heads
    shape = low_ref.shape
    row_slot = lax.broadcasted_iota(jnp.int32, shape, 0) // steps
    column = lax.broadcasted_iota(jnp.int32, shape, 1)
    first = jnp.zeros(shape, jnp.int32)
    last = jnp.zeros(shape, jnp.int32)
    for slot in range(slots_here):
        request = request_ref[me_ref[0] * slots_here + slot]
        start = adapter_ref[request] * LARGEST_RANK
        first = jnp.where(row_slot == slot, start, first)
        last = jnp.where(row_slot == slot, start + jnp.minimum(rank_ref[request], LARGEST_RANK), last)
    low = low_ref[...] + other_ref[...]
    kept = jnp.where((column >= first) & (column < last), low, 0.0).astype(jnp.bfloat16)
    raised = dot(kept, up_ref[...])
    blocks = [[None] * slots_here for _ in range(kv_heads)]
    for slot in range(slots_here):
        query = base_ref[slot].astype(jnp.float32) + raised[slot * steps : (slot + 1) * steps]
        for g in range(kv_heads):
            blocks[g][slot] = jnp.concatenate(
                [
                    query[:, (g * group + i) * HEAD_SIZE : (g * group + i + 1) * HEAD_SIZE]
                    for i in range(group)
                ],
                axis=0,
            )
    rows = group * steps
    for g in range(kv_heads):
        for slot in range(slots_here):
            b = slot * kv_heads + g
            out_ref[b * rows : (b + 1) * rows, :] = blocks[g][slot].astype(jnp.bfloat16)


def adapter_queries(kv_heads, me, request, adapter, rank, low, other, up, base, after):
    return pl.pallas_call(
        functools.partial(adapter_kernel, kv_heads),
        out_shape=jax.ShapeDtypeStruct((base.size // HEAD_SIZE, HEAD_SIZE), jnp.bfloat16),
        in_specs=[SMEM] * 4 + [VMEM] * 5,
        out_specs=VMEM,
        compiler_params=pltpu.CompilerParams(vmem_limit_bytes=8 * MIB),
        cost_estimate=pl.CostEstimate(
            flops=2 * low.shape[0] * up.size, bytes_accessed=up.size * 2, transcendentals=0
        ),
        name="adapter",
    )(me, request, adapter, rank, low, other, up, base, after)


def pin(x):
    return pltpu.with_memory_space_constraint(x, pltpu.HBM)


def exchange(x, axis, offset):
    count = lax.axis_size(axis)
    return lax.ppermute(x, axis, [(i, i ^ offset) for i in range(count)])


def gather(held, axis, bit):
    while bit:
        for offset in list(held):
            held[offset | bit] = exchange(held[offset], axis, bit)
        bit //= 2
    return held


def per_device(
    final_block_queries,
    final_block_keys,
    final_block_values,
    prompt_cached_keys,
    prompt_cached_values,
    paged_cache_pool,
    step_slot_queries,
    step_token_keys,
    step_token_values,
    normed_step_inputs,
    adapter_down_maps,
    adapter_up_maps,
    slot_request,
    request_page_table,
    lengths,
    request_adapter,
    request_rank,
):
    seq_count = lax.axis_size("seq")
    tensor_count = lax.axis_size("tensor")
    position = lax.axis_index("seq").astype(jnp.int32)
    me = position.reshape(1)
    offsets = list(range(2, seq_count)) + [1]
    half = seq_count // 2
    arrived = {half: exchange(final_block_queries, "seq", half)}

    slots_here = step_slot_queries.shape[0]
    kv_heads = final_block_keys.shape[1] // HEAD_SIZE
    request, table, lengths, request_adapter, request_rank = (
        pin(x) for x in (slot_request, request_page_table.T, lengths, request_adapter, request_rank)
    )
    low, up, base = lower(
        pin(normed_step_inputs), pin(adapter_down_maps), pin(adapter_up_maps), pin(step_slot_queries)
    )
    bit, other = 1, jnp.zeros_like(low)
    while bit < tensor_count:
        if bit > 1:
            low = low + other
        other = exchange(low, "tensor", bit)
        bit *= 2
    load = [
        pin(x)
        for x in (
            prompt_cached_keys, prompt_cached_values, final_block_keys, final_block_values,
            step_token_keys, step_token_values, final_block_queries,
        )
    ]
    pool = paged_cache_pool.reshape(*paged_cache_pool.shape[:3], kv_heads, HEAD_SIZE)
    pool = pin(pool.transpose(0, 1, 3, 2, 4))
    *loaded, pages = load_all(low, load + [pool])
    pages = pages.reshape(pages.shape[0], -1, HEAD_SIZE)
    shared, fresh, own_queries = loaded[:4], loaded[4:6], loaded[6]
    decode_queries = adapter_queries(
        kv_heads, me, request, request_adapter, request_rank, low, other, up, base, fresh[0]
    )
    arrived[half], decode_queries = lax.optimization_barrier((arrived[half], decode_queries))
    arrived = gather({0: final_block_queries} | arrived, "seq", half // 2)
    decode_arrived = {0: decode_queries}
    for o in offsets:
        decode_arrived[o] = exchange(decode_queries, "seq", o)
    returned = []
    for o in offsets:
        (part,) = prefill_part(o, me, arrived[o], *shared)
        returned.append(exchange(part, "seq", o))

    parts = decode_part(
        me, request, table, lengths, [decode_arrived[o] for o in range(seq_count)], pages, *fresh
    )
    decode_returned = [exchange(parts[1 + o], "seq", o) for o in offsets]

    prefill_out = prefill_end(own_queries, *shared, returned)
    decode_out = combine(
        decode_combine_kernel, "decode_combine", parts[0], parts[1], decode_returned,
        step_slot_queries.shape, pin(prefill_out),
    )
    return (prefill_out, decode_out)


def solution(mesh):
    placed = (
        P(("groups", "seq"), "tensor"),
        P(("groups", "seq"), "tensor"),
        P(("groups", "seq"), "tensor"),
        P(("groups", "seq"), "tensor"),
        P(("groups", "seq"), "tensor"),
        P(("groups", "seq"), None, None, "tensor"),
        P(("groups", "seq"), None, "tensor"),
        P(("groups", "seq"), None, "tensor"),
        P(("groups", "seq"), None, "tensor"),
        P(("groups", "seq"), None, "tensor"),
        P("tensor", None),
        P(None, "tensor"),
        P("groups"),
        P("groups", None),
        P("groups"),
        P("groups"),
        P("groups"),
    )
    return jax.shard_map(
        per_device,
        mesh=mesh,
        in_specs=placed,
        out_specs=(P(("groups", "seq"), "tensor"), P(("groups", "seq"), None, "tensor")),
        check_vma=False,
    )
```
